64 devices in a mesh: dp: 4 (over x, y), ep: 16 (over z, core).
Axes of the slice: x: 2, y: 2, z: 8, core: 2. Of those that a mesh axis runs over, the one named last changes fastest.
The devices are a block of a 4x4x8 slice.
Arguments:
- hidden_in: bfloat16 [6144, 2048], P(('dp', 'ep')), parts along dimension 0
- norm_gain: float32 [2048], replicated
- router_w: float32 [64, 2048], replicated
- w_gate: bfloat16 [64, 2048, 1408], P('ep')
- w_up: bfloat16 [64, 2048, 1408], P('ep')
- w_down: bfloat16 [64, 1408, 2048], P('ep')
- ws_gate: bfloat16 [2048, 2816], replicated
- ws_up: bfloat16 [2048, 2816], replicated
- ws_down: bfloat16 [2816, 2048], replicated
- expert_ids: int32 [6144, 6], P(('dp', 'ep')), parts along dimension 0
Outputs:
- output: bfloat16 [6144, 2048], P(('dp', 'ep')), parts along dimension 0
There are 4 independent parts. The reference program is written for one: setup_inputs(seed, part) draws one part's arguments, and reference() takes and returns one part's arrays. A program takes and returns all parts, laid end to end along the dimension named above; an argument that names none is the same for every part.
All inputs are finite; a program needn't handle non-finite values.
Results may differ from the reference program's by a relative error of at most 0.00428517.
Values are sent between devices in bfloat16 or wider.
A program may use at most 768 MiB of HBM per device.

```python
import jax
import jax.numpy as jnp
from jax import lax

TOKENS = 1536
D = 2048
EXPERTS = 64
INTER = 1408
SHARED_INTER = 2816
TOP = 6
GROUPS = 8
GROUP_LIMIT = 4

NORM_EPS = 1e-6
ROUTE_SCALE = 2.5
GROUP_WIDTH = EXPERTS // GROUPS
SLOT_PAIRS = (TOP + GROUP_LIMIT - 1) // GROUP_LIMIT
EXP_CAP = GROUPS * SLOT_PAIRS * TOKENS // EXPERTS


def draw_routes(route_key):
    key_hot, key_other, key_shift, key_cols = jax.random.split(route_key, 4)
    slot_sizes = [TOP // GROUP_LIMIT + int(slot_num < TOP % GROUP_LIMIT) for slot_num in range(GROUP_LIMIT)]
    slot_of_pair = jnp.array([slot_num for slot_num in range(GROUP_LIMIT) for step_num in range(slot_sizes[slot_num])], jnp.int32)
    step_of_pair = jnp.array([step_num for slot_num in range(GROUP_LIMIT) for step_num in range(slot_sizes[slot_num])], jnp.int32)
    hot_group = jax.random.randint(key_hot, (), 0, GROUPS).astype(jnp.int32)
    other_scores = jax.random.randint(key_other, (TOKENS, GROUPS - 1), 0, 1 << 20).astype(jnp.int32) * (GROUPS - 1) + jnp.arange(GROUPS - 1, dtype=jnp.int32)
    other_offsets = jnp.argsort(other_scores, axis=1)[:, : GROUP_LIMIT - 1].astype(jnp.int32)
    token_groups = jnp.concatenate([jnp.zeros((TOKENS, 1), jnp.int32) + hot_group, (hot_group + 1 + other_offsets) % GROUPS], axis=1)
    pair_groups = token_groups[:, slot_of_pair]
    group_shift = jax.random.randint(key_shift, (GROUPS,), 0, GROUP_WIDTH).astype(jnp.int32)
    token_pos = jnp.arange(TOKENS, dtype=jnp.int32)[:, None]
    within = (token_pos + step_of_pair[None, :] + group_shift[pair_groups]) % GROUP_WIDTH
    routes = pair_groups * GROUP_WIDTH + within
    col_scores = jax.random.randint(key_cols, (TOKENS, TOP), 0, 1 << 20).astype(jnp.int32) * TOP + jnp.arange(TOP, dtype=jnp.int32)
    col_order = jnp.argsort(col_scores, axis=1)
    return jnp.take_along_axis(routes, col_order, axis=1).astype(jnp.int32)


def setup_inputs(seed: int = 0, part: int = 0) -> dict:
    base_key = jax.random.key(seed)
    weight_keys = jax.random.split(base_key, 9)
    part_keys = jax.random.split(jax.random.fold_in(base_key, part), 2)
    hidden_in = jax.random.normal(part_keys[0], (TOKENS, D), jnp.float32).astype(jnp.bfloat16)
    expert_ids = draw_routes(part_keys[1])
    norm_gain = jax.random.uniform(weight_keys[0], (D,), jnp.float32, 0.5, 1.5)
    router_w = jax.random.normal(weight_keys[1], (EXPERTS, D), jnp.float32) * D ** -0.5
    w_gate = (jax.random.normal(weight_keys[2], (EXPERTS, D, INTER), jnp.float32) * D ** -0.5).astype(jnp.bfloat16)
    w_up = (jax.random.normal(weight_keys[3], (EXPERTS, D, INTER), jnp.float32) * D ** -0.5).astype(jnp.bfloat16)
    out_scale = jax.random.uniform(weight_keys[4], (EXPERTS, 1, 1), jnp.float32, 1.0, 3.0)
    w_down = (jax.random.normal(weight_keys[5], (EXPERTS, INTER, D), jnp.float32) * INTER ** -0.5 * out_scale).astype(jnp.bfloat16)
    ws_gate = (jax.random.normal(weight_keys[6], (D, SHARED_INTER), jnp.float32) * D ** -0.5).astype(jnp.bfloat16)
    ws_up = (jax.random.normal(weight_keys[7], (D, SHARED_INTER), jnp.float32) * D ** -0.5).astype(jnp.bfloat16)
    ws_down = (jax.random.normal(weight_keys[8], (SHARED_INTER, D), jnp.float32) * SHARED_INTER ** -0.5).astype(jnp.bfloat16)
    return {"hidden_in": hidden_in, "norm_gain": norm_gain, "router_w": router_w, "w_gate": w_gate, "w_up": w_up, "w_down": w_down, "ws_gate": ws_gate, "ws_up": ws_up, "ws_down": ws_down, "expert_ids": expert_ids}


def swiglu(tok_rows, gate_mat, up_mat, down_mat):
    h_gate = jnp.dot(tok_rows, gate_mat, preferred_element_type=jnp.float32)
    h_up = jnp.dot(tok_rows, up_mat, preferred_element_type=jnp.float32)
    hidden = (jax.nn.silu(h_gate) * h_up).astype(jnp.bfloat16)
    return jnp.dot(hidden, down_mat, preferred_element_type=jnp.float32).astype(jnp.bfloat16)


def reference(hidden_in, norm_gain, router_w, w_gate, w_up, w_down, ws_gate, ws_up, ws_down, expert_ids):
    x_f32 = hidden_in.astype(jnp.float32)
    inv_rms = lax.rsqrt(jnp.mean(x_f32 * x_f32, axis=1, keepdims=True) + NORM_EPS)
    x_norm = (x_f32 * inv_rms * norm_gain).astype(jnp.bfloat16)
    scores = jax.nn.sigmoid(jnp.dot(x_norm.astype(jnp.float32), router_w.T))
    picked = jnp.take_along_axis(scores, expert_ids, axis=1)
    gate_vals = ROUTE_SCALE * picked / jnp.sum(picked, axis=1, keepdims=True)
    flat_ids = expert_ids.reshape(-1)
    pair_tok = jnp.arange(TOKENS * TOP, dtype=jnp.int32) // TOP
    sort_order = jnp.argsort(flat_ids)
    counts = jnp.bincount(flat_ids, length=EXPERTS).astype(jnp.int32)
    starts = jnp.cumsum(counts) - counts
    sorted_tok = jnp.concatenate([pair_tok[sort_order], jnp.full((EXP_CAP,), TOKENS, jnp.int32)])
    norm_pad = jnp.concatenate([x_norm, jnp.zeros((1, D), x_norm.dtype)], axis=0)

    def one_expert(expert_xs):
        gate_mat, up_mat, down_mat, row_start, row_count = expert_xs
        row_tok = lax.dynamic_slice(sorted_tok, (row_start,), (EXP_CAP,))
        row_tok = jnp.where(jnp.arange(EXP_CAP, dtype=jnp.int32) < row_count, row_tok, TOKENS)
        return swiglu(norm_pad[row_tok], gate_mat, up_mat, down_mat)

    expert_out = lax.map(one_expert, (w_gate, w_up, w_down, starts, counts))
    sorted_rank = (jnp.arange(TOKENS * TOP, dtype=jnp.int32) - starts[flat_ids[sort_order]]).astype(jnp.int32)
    pair_rank = jnp.zeros((TOKENS * TOP,), jnp.int32).at[sort_order].set(sorted_rank)
    pair_out = expert_out[flat_ids, pair_rank].reshape(TOKENS, TOP, D)
    routed = jnp.sum(gate_vals[:, :, None] * pair_out.astype(jnp.float32), axis=1)
    shared_out = swiglu(x_norm, ws_gate, ws_up, ws_down)
    return (x_f32 + shared_out.astype(jnp.float32) + routed).astype(jnp.bfloat16)
```

```python
import functools

import jax
import jax.numpy as jnp
from jax import lax
from jax.experimental import pallas as pl
from jax.experimental.pallas import tpu as pltpu
from jax.sharding import PartitionSpec as P

NORM_EPS = 1e-6
ROUTE_SCALE = 2.5
GROUPS = 8
GROUP_LIMIT = 4
LANES = 128
COLS = 256
STREAM_SLOTS = 6
MESH = pl.DeviceIdType.MESH
F32 = jnp.float32
BF16 = jnp.bfloat16


def moe_kernel(
    ep_size,
    cap,
    hidden_ref,
    gain_ref,
    router_ref,
    ids_ref,
    wg_hbm,
    wu_hbm,
    wd_hbm,
    sg_hbm,
    su_hbm,
    sd_hbm,
    out_ref,
    xbuf,
    gsend,
    gmsg,
    rank_ref,
    cols_ref,
    pick,
    place,
    xg,
    hid,
    shid,
    sout,
    wbuf,
    dbuf,
    part,
    erows,
    from_core,
    ring,
    w_sem,
    d_sem,
    ag_send,
    ag_recv,
    cc_send,
    cc_recv,
    g_send,
    g_recv,
    p_send,
    p_recv,
    r_send,
    r_recv,
):
    tok, dim = hidden_ref.shape
    half = tok // 2
    top_k = ids_ref.shape[1]
    n_exp = wg_hbm.shape[0]
    inter = wg_hbm.shape[2]
    s_inter = sg_hbm.shape[1]
    chips = ep_size // 2
    far = chips // 2
    own_pos = chips - 2
    far_pos = chips - 1
    n_groups = chips // 2
    group_rows = 4 * tok
    tiles_per_group = group_rows // LANES
    n_chunks = dim // COLS
    slots = n_exp * cap
    sh_steps = s_inter // LANES
    ex_steps = inter // LANES
    w_steps = sh_steps + n_exp * ex_steps
    d_per = n_exp + 2

    me = lax.axis_index("ep")
    core = lax.rem(me, 2)
    chip = me // 2
    partner = chip * 2 + (1 - core)

    def at_chip(delta, which):
        return lax.rem(chip + delta + chips, chips) * 2 + which

    def pos_of(way, hops):
        return far_pos if hops == far else 2 * (hops - 1) + way

    def pos_at(delta):
        if delta == 0:
            return own_pos
        if abs(delta) == far:
            return far_pos
        return pos_of(0, delta) if delta > 0 else pos_of(1, -delta)

    def row_at(pos, which):
        return pos * 2 * tok + which * tok

    def w_pair(step):
        slot = lax.rem(step, STREAM_SLOTS)
        return slot

    def w_copies_shared(step):
        slot = w_pair(step)
        col = pl.ds(pl.multiple_of(step * LANES, LANES), LANES)
        return (
            pltpu.make_async_copy(sg_hbm.at[:, col], wbuf.at[slot, :, pl.ds(0, LANES)], w_sem.at[slot, 0]),
            pltpu.make_async_copy(su_hbm.at[:, col], wbuf.at[slot, :, pl.ds(LANES, LANES)], w_sem.at[slot, 1]),
        )

    def w_copies_expert(step):
        slot = w_pair(step)
        rel = step - sh_steps
        exp = rel // ex_steps
        col = pl.ds(pl.multiple_of((rel - exp * ex_steps) * LANES, LANES), LANES)
        return (
            pltpu.make_async_copy(wg_hbm.at[exp, :, col], wbuf.at[slot, :, pl.ds(0, LANES)], w_sem.at[slot, 0]),
            pltpu.make_async_copy(wu_hbm.at[exp, :, col], wbuf.at[slot, :, pl.ds(LANES, LANES)], w_sem.at[slot, 1]),
        )

    def w_start(step):
        @pl.when(step < sh_steps)
        def _():
            for copy in w_copies_shared(step):
                copy.start()

        @pl.when((step >= sh_steps) & (step < w_steps))
        def _():
            for copy in w_copies_expert(step):
                copy.start()

    def d_copy(chunk, which):
        slot = lax.rem(chunk, 2) * d_per + which
        col = pl.ds(pl.multiple_of(chunk * COLS, COLS), COLS)
        if which < n_exp:
            src = wd_hbm.at[which, :, col]
        else:
            src = sd_hbm.at[pl.ds((which - n_exp) * inter, inter), col]
        return pltpu.make_async_copy(src, dbuf.at[slot], d_sem.at[slot])

    def ag_copy(way, hops, u):
        src_row = row_at(own_pos if hops == 1 else pos_of(way, hops - 1), core) + u * half
        dst_row = row_at(pos_of(way, hops), core) + u * half
        return pltpu.make_async_remote_copy(
            src_ref=xbuf.at[pl.ds(src_row, half), :],
            dst_ref=xbuf.at[pl.ds(dst_row, half), :],
            send_sem=ag_send.at[way, hops - 1, u],
            recv_sem=ag_recv.at[way, hops - 1, u],
            device_id={"ep": at_chip(1 if way == 0 else -1, core)},
            device_id_type=MESH,
        )

    def cc_copy(way, hops, u, which):
        pos = own_pos if hops == 0 else pos_of(way, hops)
        rows = pl.ds(row_at(pos, which) + u * half, half)
        return pltpu.make_async_remote_copy(
            src_ref=xbuf.at[rows, :],
            dst_ref=xbuf.at[rows, :],
            send_sem=cc_send.at[way, hops, u],
            recv_sem=cc_recv.at[way, hops, u],
            device_id={"ep": partner},
            device_id_type=MESH,
        )

    def halves(way, hops):
        if hops == far:
            return (way,)
        return (0, 1) if way == 0 else (1, 0)

    def relay(hops, nth):
        for way in (0, 1):
            if nth >= len(halves(way, hops)):
                continue
            u = halves(way, hops)[nth]
            ag_copy(way, hops, u).wait_recv()
            if hops < far and u in halves(way, hops + 1):
                ag_copy(way, hops + 1, u).start()
            cc_copy(way, hops, u, core).start()

    def gate_copy(delta, other):
        dst_pos = pos_at(delta)
        dest = partner if delta == 0 else at_chip(delta, core if other == 0 else 1 - core)
        return pltpu.make_async_remote_copy(
            src_ref=gsend.at[dest],
            dst_ref=gmsg.at[dst_pos, core],
            send_sem=g_send.at[dst_pos, other],
            recv_sem=g_recv.at[dst_pos, core],
            device_id={"ep": dest},
            device_id_type=MESH,
        )

    deltas = [d for d in range(-(far - 1), far + 1)]

    for step in range(STREAM_SLOTS):
        w_start(jnp.int32(step))
    barrier = pltpu.get_barrier_semaphore()
    for off in range(1, ep_size):
        pl.semaphore_signal(barrier, inc=1, device_id={"ep": lax.rem(me + off, ep_size)}, device_id_type=MESH)

    x_f32 = hidden_ref[...].astype(F32)
    inv_rms = lax.rsqrt(jnp.mean(x_f32 * x_f32, axis=-1, keepdims=True) + NORM_EPS)
    x_norm = (x_f32 * inv_rms * gain_ref[...]).astype(BF16)
    own_row = row_at(own_pos, core)
    xbuf[pl.ds(pl.multiple_of(own_row, tok), tok), :] = x_norm

    pl.semaphore_wait(barrier, ep_size - 1)
    for nth in (0, 1):
        for way in (0, 1):
            ag_copy(way, 1, halves(way, 1)[nth]).start()
    for u in (0, 1):
        cc_copy(0, 0, u, core).start()

    logits = lax.dot_general(
        x_norm.astype(F32),
        router_ref[...],
        (((1,), (1,)), ((), ())),
        precision=lax.Precision.HIGHEST,
        preferred_element_type=F32,
    )
    scores = jax.nn.sigmoid(logits)
    exp_iota = lax.broadcasted_iota(jnp.int32, scores.shape, 1)
    chosen = exp_iota == ids_ref[:, 0:1]
    for k in range(1, top_k):
        chosen = chosen | (exp_iota == ids_ref[:, k : k + 1])
    total = jnp.sum(jnp.where(chosen, scores, 0.0), axis=1, keepdims=True)
    gates = jnp.where(chosen, ROUTE_SCALE * scores / total, -1.0)
    n_all = gates.shape[1]
    gates = jnp.concatenate([gates, jnp.full((tok, LANES - n_all), -1.0, F32)], axis=1)
    gates = jnp.concatenate([gates, jnp.full((LANES - tok, LANES), -1.0, F32)], axis=0)
    gates_t = jnp.transpose(gates)
    for dest in range(ep_size):
        piece = gates_t[dest * n_exp : (dest + 1) * n_exp, :]
        gsend[dest] = jnp.concatenate([piece, jnp.full((8 - n_exp, LANES), -1.0, F32)], axis=0)
    gmsg[own_pos, core] = gsend[me]
    for delta in deltas:
        for other in (0, 1):
            if delta == 0 and other == 0:
                continue
            gate_copy(delta, other).start()

    for chunk in (0, 1):
        for which in range(d_per):
            d_copy(jnp.int32(chunk), which).start()

    def shared_step(step, carry):
        slot = w_pair(step)
        for copy in w_copies_shared(step):
            copy.wait()
        x_own = xbuf[pl.ds(pl.multiple_of(own_row, tok), tok), :]
        both = jnp.dot(x_own, wbuf[slot], preferred_element_type=F32)
        act = (jax.nn.silu(both[:, :LANES]) * both[:, LANES:]).astype(BF16)
        shid[:, pl.ds(pl.multiple_of(step * LANES, LANES), LANES)] = act
        w_start(step + STREAM_SLOTS)
        return carry

    split = sh_steps // 2
    lax.fori_loop(0, split, shared_step, 0)
    relay(1, 0)
    lax.fori_loop(split, sh_steps, shared_step, 0)
    relay(1, 1)

    for delta in deltas:
        for other in (0, 1):
            if delta == 0 and other == 0:
                continue
            if delta == 0:
                src_pos, src_core = own_pos, 1 - core
            else:
                src_pos = pos_at(delta)
                src_core = core if other == 0 else 1 - core
            pltpu.make_async_remote_copy(
                src_ref=gsend.at[0],
                dst_ref=gmsg.at[src_pos, src_core],
                send_sem=g_send.at[src_pos, other],
                recv_sem=g_recv.at[src_pos, src_core],
                device_id={"ep": partner},
                device_id_type=MESH,
            ).wait_recv()

    lane = lax.broadcasted_iota(jnp.int32, (8, LANES), 1)
    packed = []
    for g in range(n_groups):
        b0, b1, b2, b3 = gmsg[2 * g, 0], gmsg[2 * g, 1], gmsg[2 * g + 1, 0], gmsg[2 * g + 1, 1]
        r1 = pltpu.roll(b1, 96, 1)
        r2 = pltpu.roll(b2, 64, 1)
        r3 = pltpu.roll(b3, 32, 1)
        packed.append(jnp.where(lane < 96, b0, r1))
        packed.append(jnp.where(lane < 64, r1, r2))
        packed.append(jnp.where(lane < 32, r2, r3))
    n_tiles = len(packed)
    member = jnp.concatenate([jnp.where(p < 0, 0.0, 1.0) for p in packed], axis=0)
    upper = jnp.where(
        lax.broadcasted_iota(jnp.int32, (LANES, LANES), 0) < lax.broadcasted_iota(jnp.int32, (LANES, LANES), 1), 1.0, 0.0
    ).astype(BF16)
    within = jnp.dot(member.astype(BF16), upper, preferred_element_type=F32)
    base = jnp.zeros((8, 1), F32)
    for t in range(n_tiles):
        m = member[t * 8 : (t + 1) * 8]
        rank = jnp.where(m > 0, within[t * 8 : (t + 1) * 8] + base, -1.0)
        base = base + jnp.sum(m, axis=1, keepdims=True)
        rank_ref[t] = rank
        both = jnp.concatenate([rank, packed[t], jnp.zeros((LANES - 16, LANES), F32)], axis=0)
        cols_ref[t * LANES : (t + 1) * LANES, :] = jnp.transpose(both)

    slot_rows = lax.broadcasted_iota(jnp.int32, (cap, LANES), 0).astype(F32)
    slot_lanes = lax.broadcasted_iota(jnp.int32, (LANES, cap), 1).astype(F32)

    def build(t, carry):
        rank = rank_ref[t]
        col = cols_ref[pl.ds(pl.multiple_of(t * LANES, LANES), LANES), :]
        for e in range(n_exp):
            hot = jnp.where(slot_rows == rank[e : e + 1, :], 1.0, 0.0)
            pick[e * cap : (e + 1) * cap, pl.ds(pl.multiple_of(t * LANES, LANES), LANES)] = hot.astype(BF16)
            hot_t = jnp.where(slot_lanes == col[:, e : e + 1], 1.0, 0.0)
            place[pl.ds(pl.multiple_of(t * LANES, LANES), LANES), e * cap : (e + 1) * cap] = hot_t.astype(BF16)
        return carry

    lax.fori_loop(0, n_tiles, build, 0)

    def gather_group(g):
        def body(n, carry):
            cols = pl.ds(pl.multiple_of(n * COLS, COLS), COLS)
            rows = xbuf[g * group_rows : (g + 1) * group_rows, cols]
            for e in range(n_exp):
                hot = pick[e * cap : (e + 1) * cap, g * group_rows : (g + 1) * group_rows]
                got = jnp.dot(hot, rows, preferred_element_type=F32).astype(BF16)
                if g > 0:
                    got = got + xg[e * cap : (e + 1) * cap, cols]
                xg[e * cap : (e + 1) * cap, cols] = got
            return carry

        lax.fori_loop(0, n_chunks, body, 0)

    def wait_from_core(hops):
        for way in (0, 1):
            if hops == 0 and way == 1:
                continue
            for u in (0, 1) if hops == 0 else halves(way, hops):
                cc_copy(way, hops, u, 1 - core).wait_recv()

    relay(2, 0)
    wait_from_core(1)
    gather_group(0)
    relay(2, 1)
    relay(3, 0)
    wait_from_core(2)
    gather_group(1)
    relay(3, 1)
    wait_from_core(3)
    relay(4, 0)
    gather_group(2)
    wait_from_core(0)
    wait_from_core(4)
    gather_group(3)

    def up_step(step, carry):
        slot = w_pair(step)
        for copy in w_copies_expert(step):
            copy.wait()
        rel = step - sh_steps
        exp = rel // ex_steps
        j = rel - exp * ex_steps
        rows = pl.ds(pl.multiple_of(exp * cap, cap), cap)
        both = jnp.dot(xg[rows, :], wbuf[slot], preferred_element_type=F32)
        act = (jax.nn.silu(both[:, :LANES]) * both[:, LANES:]).astype(BF16)
        hid[rows, pl.ds(pl.multiple_of(j * LANES, LANES), LANES)] = act
        w_start(step + STREAM_SLOTS)
        return carry

    lax.fori_loop(sh_steps, w_steps, up_step, 0)

    def part_copy(chunk):
        par = lax.rem(chunk, 2)
        return pltpu.make_async_remote_copy(
            src_ref=part.at[par, :, 1 - core],
            dst_ref=from_core.at[chunk],
            send_sem=p_send.at[chunk],
            recv_sem=p_recv.at[chunk],
            device_id={"ep": partner},
            device_id_type=MESH,
        )

    def ring_copy(chunk, way, hop):
        dev = {"ep": at_chip(1 if way == 0 else -1, core)}
        if hop == 1:
            src = from_core.at[chunk, far_pos, pl.ds(way * half, half), :]
            dst = ring.at[chunk, way, 0, pl.ds(way * half, half), :]
        else:
            src = ring.at[chunk, way, hop - 2]
            dst = ring.at[chunk, way, hop - 1]
        return pltpu.make_async_remote_copy(
            src_ref=src,
            dst_ref=dst,
            send_sem=r_send.at[chunk, way, hop - 1],
            recv_sem=r_recv.at[chunk, way, hop - 1],
            device_id=dev,
            device_id_type=MESH,
        )

    def dest_pos(way, hops):
        return pos_of(1 - way, hops)

    def compute(chunk):
        par = lax.rem(chunk, 2)
        cols = pl.ds(pl.multiple_of(chunk * COLS, COLS), COLS)
        for e in range(n_exp):
            d_copy(chunk, e).wait()
            got = jnp.dot(hid[e * cap : (e + 1) * cap, :], dbuf[par * d_per + e], preferred_element_type=F32)
            erows[e * cap : (e + 1) * cap, :] = got.astype(BF16)
        for k in range(2):
            d_copy(chunk, n_exp + k).wait()
        shared = jnp.dot(shid[:, :inter], dbuf[par * d_per + n_exp], preferred_element_type=F32)
        shared = shared + jnp.dot(shid[:, inter:], dbuf[par * d_per + n_exp + 1], preferred_element_type=F32)
        sout[:, cols] = shared.astype(BF16)

        @pl.when(chunk + 2 < n_chunks)
        def _():
            for which in range(d_per):
                d_copy(chunk + 2, which).start()

        @pl.when(chunk >= 2)
        def _():
            part_copy(chunk - 2).wait_send()

        def combine(g, carry):
            rows = pl.ds(pl.multiple_of(g * group_rows, group_rows), group_rows)
            acc = None
            for e in range(n_exp):
                got = jnp.dot(
                    place[rows, e * cap : (e + 1) * cap], erows[e * cap : (e + 1) * cap, :], preferred_element_type=F32
                )
                got = cols_ref[rows, 8 + e : 9 + e] * got
                acc = got if acc is None else acc + got
            for b in range(4):
                part[par, 2 * g + b // 2, b % 2] = acc[b * tok : (b + 1) * tok]
            return carry

        lax.fori_loop(0, n_groups, combine, 0)
        part_copy(chunk).start()

    def fold(chunk):
        par = lax.rem(chunk, 2)
        part_copy(chunk).wait_recv()
        for pos in range(chips):
            from_core[chunk, pos] = from_core[chunk, pos] + part[par, pos, core]
        for way in (0, 1):
            ring_copy(chunk, way, 1).start()

    def pass_on(chunk, hop):
        for way in (0, 1):
            ring_copy(chunk, way, hop).wait_recv()
            pos = dest_pos(way, far - hop)
            if hop == 1:
                done = pl.ds(way * half, half)
                rest = pl.ds((1 - way) * half, half)
                ring[chunk, way, 0, done, :] = ring[chunk, way, 0, done, :] + from_core[chunk, pos, done, :]
                ring[chunk, way, 0, rest, :] = from_core[chunk, pos, rest, :]
            else:
                ring[chunk, way, hop - 1] = ring[chunk, way, hop - 1] + from_core[chunk, pos]
            ring_copy(chunk, way, hop + 1).start()

    def finish(chunk):
        cols = pl.ds(pl.multiple_of(chunk * COLS, COLS), COLS)
        for way in (0, 1):
            ring_copy(chunk, way, far).wait_recv()
        routed = from_core[chunk, own_pos] + ring[chunk, 0, far - 1] + ring[chunk, 1, far - 1]
        out_ref[:, cols] = (hidden_ref[:, cols].astype(F32) + sout[:, cols].astype(F32) + routed).astype(BF16)

    def turn(i, carry):
        @pl.when(i < n_chunks)
        def _():
            compute(i)

        @pl.when((i >= far) & (i - far < n_chunks))
        def _():
            finish(i - far)

        for hop in range(far - 1, 0, -1):
            @pl.when((i >= hop) & (i - hop < n_chunks))
            def _():
                pass_on(i - hop, hop)

        @pl.when(i < n_chunks)
        def _():
            fold(i)

        return carry

    lax.fori_loop(0, n_chunks + far, turn, 0)

    for hops in range(1, far + 1):
        for way in (0, 1):
            for u in halves(way, hops):
                ag_copy(way, hops, u).wait_send()
                cc_copy(way, hops, u, core).wait_send()
    for u in (0, 1):
        cc_copy(0, 0, u, core).wait_send()
    for delta in deltas:
        for other in (0, 1):
            if not (delta == 0 and other == 0):
                gate_copy(delta, other).wait_send()

    def drain(chunk, carry):
        @pl.when(chunk >= n_chunks - 2)
        def _():
            part_copy(chunk).wait_send()

        for way in (0, 1):
            for hop in range(1, far + 1):
                ring_copy(chunk, way, hop).wait_send()
        return carry

    lax.fori_loop(0, n_chunks, drain, 0)


def solution(mesh):
    ep_size = mesh.shape["ep"]

    def local_block(hidden_in, norm_gain, router_w, w_gate, w_up, w_down, ws_gate, ws_up, ws_down, expert_ids):
        tok, top_k = expert_ids.shape
        dim = hidden_in.shape[1]
        n_exp, _, inter = w_gate.shape
        s_inter = ws_gate.shape[1]
        chips = ep_size // 2
        far = chips // 2
        n_chunks = dim // COLS
        pair_cap = GROUPS * ((top_k + GROUP_LIMIT - 1) // GROUP_LIMIT) * tok // ep_size
        cap = pair_cap * ep_size // n_exp
        all_tok = ep_size * tok
        slots = n_exp * cap
        n_tiles = all_tok // LANES
        vmem = pl.BlockSpec(memory_space=pltpu.VMEM)
        hbm = pl.BlockSpec(memory_space=pl.ANY)
        dma = pltpu.SemaphoreType.DMA
        return pl.pallas_call(
            functools.partial(moe_kernel, ep_size, cap),
            out_shape=jax.ShapeDtypeStruct((tok, dim), BF16),
            in_specs=[vmem] * 4 + [hbm] * 6,
            out_specs=vmem,
            scratch_shapes=[
                pltpu.VMEM((all_tok, dim), BF16),
                pltpu.VMEM((ep_size, 8, LANES), F32),
                pltpu.VMEM((chips, 2, 8, LANES), F32),
                pltpu.VMEM((n_tiles, 8, LANES), F32),
                pltpu.VMEM((all_tok, LANES), F32),
                pltpu.VMEM((slots, all_tok), BF16),
                pltpu.VMEM((all_tok, slots), BF16),
                pltpu.VMEM((slots, dim), BF16),
                pltpu.VMEM((slots, inter), BF16),
                pltpu.VMEM((tok, s_inter), BF16),
                pltpu.VMEM((tok, dim), BF16),
                pltpu.VMEM((STREAM_SLOTS, dim, 2 * LANES), BF16),
                pltpu.VMEM((2 * (n_exp + 2), inter, COLS), BF16),
                pltpu.VMEM((2, chips, 2, tok, COLS), F32),
                pltpu.VMEM((slots, COLS), BF16),
                pltpu.VMEM((n_chunks, chips, tok, COLS), F32),
                pltpu.VMEM((n_chunks, 2, far, tok, COLS), F32),
                dma((STREAM_SLOTS, 2)),
                dma((2 * (n_exp + 2),)),
                dma((2, far, 2)),
                dma((2, far, 2)),
                dma((2, far + 1, 2)),
                dma((2, far + 1, 2)),
                dma((chips, 2)),
                dma((chips, 2)),
                dma((n_chunks,)),
                dma((n_chunks,)),
                dma((n_chunks, 2, far)),
                dma((n_chunks, 2, far)),
            ],
            compiler_params=pltpu.CompilerParams(
                collective_id=0, has_side_effects=True, vmem_limit_bytes=67043328
            ),
        )(hidden_in, norm_gain.reshape(1, dim), router_w, expert_ids, w_gate, w_up, w_down, ws_gate, ws_up, ws_down)

    row_spec = P(("dp", "ep"), None)
    in_specs = (row_spec, P(), P(), P("ep"), P("ep"), P("ep"), P(), P(), P(), row_spec)
    return jax.shard_map(local_block, mesh=mesh, in_specs=in_specs, out_specs=row_spec, check_vma=False)
```

```python
import functools

import jax
import jax.numpy as jnp
from jax import lax
from jax.experimental import pallas as pl
from jax.experimental.pallas import tpu as pltpu
from jax.sharding import PartitionSpec as P

NORM_EPS = 1e-6
ROUTE_SCALE = 2.5
GROUPS = 8
GROUP_LIMIT = 4
LANES = 128
COLS = 256
STREAM_SLOTS = 8
STEP_UNITS = 4
MESH = pl.DeviceIdType.MESH
F32 = jnp.float32
BF16 = jnp.bfloat16


def moe_kernel(
    ep_size,
    cap,
    hidden_ref,
    gain_ref,
    router_ref,
    ids_ref,
    wg_hbm,
    wu_hbm,
    wd_hbm,
    sg_hbm,
    su_hbm,
    sd_hbm,
    out_ref,
    xbuf,
    gsend,
    gmsg,
    rank_ref,
    cols_ref,
    pick,
    place,
    xg,
    hid,
    shid,
    sout,
    wbuf,
    dbuf,
    part,
    erows,
    from_core,
    ring,
    w_sem,
    d_sem,
    ag_send,
    ag_recv,
    cc_send,
    cc_recv,
    g_send,
    g_recv,
    p_send,
    p_recv,
    r_send,
    r_recv,
):
    tok, dim = hidden_ref.shape
    half = tok // 2
    top_k = ids_ref.shape[0]
    n_exp = wg_hbm.shape[0]
    inter = wg_hbm.shape[2]
    s_inter = sg_hbm.shape[1]
    chips = ep_size // 2
    far = chips // 2
    own_pos = 0
    far_pos = chips - 1
    n_groups = chips // 2
    group_rows = 4 * tok
    tiles_per_group = group_rows // LANES
    n_chunks = dim // COLS
    slots = n_exp * cap
    sh_steps = s_inter // LANES
    ex_steps = inter // LANES
    w_steps = sh_steps + n_exp * ex_steps
    d_per = n_exp + 2

    me = lax.axis_index("ep")
    core = lax.rem(me, 2)
    chip = me // 2
    partner = chip * 2 + (1 - core)

    def at_chip(delta, which):
        return lax.rem(chip + delta + chips, chips) * 2 + which

    def pos_of(way, hops):
        return far_pos if hops == far else 2 * hops - 1 + way

    def pos_at(delta):
        if delta == 0:
            return own_pos
        if abs(delta) == far:
            return far_pos
        return pos_of(0, delta) if delta > 0 else pos_of(1, -delta)

    def row_at(pos, which):
        return pos * 2 * tok + which * tok

    def w_pair(step):
        slot = lax.rem(step, STREAM_SLOTS)
        return slot

    def w_copies_shared(step):
        slot = w_pair(step)
        col = pl.ds(pl.multiple_of(step * LANES, LANES), LANES)
        return (
            pltpu.make_async_copy(sg_hbm.at[:, col], wbuf.at[slot, :, pl.ds(0, LANES)], w_sem.at[slot, 0]),
            pltpu.make_async_copy(su_hbm.at[:, col], wbuf.at[slot, :, pl.ds(LANES, LANES)], w_sem.at[slot, 1]),
        )

    def w_copies_expert(step):
        slot = w_pair(step)
        rel = step - sh_steps
        exp = rel // ex_steps
        col = pl.ds(pl.multiple_of((rel - exp * ex_steps) * LANES, LANES), LANES)
        return (
            pltpu.make_async_copy(wg_hbm.at[exp, :, col], wbuf.at[slot, :, pl.ds(0, LANES)], w_sem.at[slot, 0]),
            pltpu.make_async_copy(wu_hbm.at[exp, :, col], wbuf.at[slot, :, pl.ds(LANES, LANES)], w_sem.at[slot, 1]),
        )

    def w_start(step):
        @pl.when(step < sh_steps)
        def _():
            for copy in w_copies_shared(step):
                copy.start()

        @pl.when((step >= sh_steps) & (step < w_steps))
        def _():
            for copy in w_copies_expert(step):
                copy.start()

    def d_copy(chunk, which):
        slot = lax.rem(chunk, 2) * d_per + which
        col = pl.ds(pl.multiple_of(chunk * COLS, COLS), COLS)
        if which < n_exp:
            src = wd_hbm.at[which, :, col]
        else:
            src = sd_hbm.at[pl.ds((which - n_exp) * inter, inter), col]
        return pltpu.make_async_copy(src, dbuf.at[slot], d_sem.at[slot])

    def ag_copy(way, hops, u):
        src_row = row_at(own_pos if hops == 1 else pos_of(way, hops - 1), core) + u * half
        dst_row = row_at(pos_of(way, hops), core) + u * half
        return pltpu.make_async_remote_copy(
            src_ref=xbuf.at[pl.ds(src_row, half), :],
            dst_ref=xbuf.at[pl.ds(dst_row, half), :],
            send_sem=ag_send.at[way, hops - 1, u],
            recv_sem=ag_recv.at[way, hops - 1, u],
            device_id={"ep": at_chip(1 if way == 0 else -1, core)},
            device_id_type=MESH,
        )

    def cc_copy(way, hops, u, which):
        pos = own_pos if hops == 0 else pos_of(way, hops)
        rows = pl.ds(row_at(pos, which) + u * half, half)
        return pltpu.make_async_remote_copy(
            src_ref=xbuf.at[rows, :],
            dst_ref=xbuf.at[rows, :],
            send_sem=cc_send.at[way, hops, u],
            recv_sem=cc_recv.at[way, hops, u],
            device_id={"ep": partner},
            device_id_type=MESH,
        )

    def halves(way, hops):
        if hops == far:
            return (way,)
        return (0, 1) if way == 0 else (1, 0)

    def relay(hops, nth):
        for way in (0, 1):
            if nth >= len(halves(way, hops)):
                continue
            u = halves(way, hops)[nth]
            ag_copy(way, hops, u).wait_recv()
            if hops < far and u in halves(way, hops + 1):
                ag_copy(way, hops + 1, u).start()
            cc_copy(way, hops, u, core).start()

    def gate_copy(delta, other):
        dst_pos = pos_at(delta)
        dest = partner if delta == 0 else at_chip(delta, core if other == 0 else 1 - core)
        return pltpu.make_async_remote_copy(
            src_ref=gsend.at[dest],
            dst_ref=gmsg.at[dst_pos, core],
            send_sem=g_send.at[dst_pos, other],
            recv_sem=g_recv.at[dst_pos, core],
            device_id={"ep": dest},
            device_id_type=MESH,
        )

    deltas = [d for d in range(-(far - 1), far + 1)]

    for step in range(STREAM_SLOTS):
        w_start(jnp.int32(step))
    barrier = pltpu.get_barrier_semaphore()
    for off in range(1, ep_size):
        pl.semaphore_signal(barrier, inc=1, device_id={"ep": lax.rem(me + off, ep_size)}, device_id_type=MESH)

    x_f32 = hidden_ref[...].astype(F32)
    inv_rms = lax.rsqrt(jnp.mean(x_f32 * x_f32, axis=-1, keepdims=True) + NORM_EPS)
    x_norm = (x_f32 * inv_rms * gain_ref[...]).astype(BF16)
    own_row = row_at(own_pos, core)
    xbuf[pl.ds(pl.multiple_of(own_row, tok), tok), :] = x_norm

    with jax.named_scope("barrier"):
        pl.semaphore_wait(barrier, ep_size - 1)
    for nth in (0, 1):
        for way in (0, 1):
            ag_copy(way, 1, halves(way, 1)[nth]).start()
    for u in (0, 1):
        cc_copy(0, 0, u, core).start()

    with jax.named_scope("gates"):
        logits = lax.dot_general(
            router_ref[...],
            x_norm.astype(F32),
            (((1,), (1,)), ((), ())),
            precision=lax.Precision.HIGHEST,
            preferred_element_type=F32,
        )
        scores = jax.nn.sigmoid(logits)
        exp_iota = lax.broadcasted_iota(jnp.int32, scores.shape, 0)
        chosen = exp_iota == ids_ref[0:1, :]
        for k in range(1, top_k):
            chosen = chosen | (exp_iota == ids_ref[k : k + 1, :])
        total = jnp.sum(jnp.where(chosen, scores, 0.0), axis=0, keepdims=True)
        gates = jnp.where(chosen, ROUTE_SCALE * scores / total, -1.0)
        gates_t = jnp.concatenate([gates, jnp.full((gates.shape[0], LANES - tok), -1.0, F32)], axis=1)
        for dest in range(ep_size):
            piece = gates_t[dest * n_exp : (dest + 1) * n_exp, :]
            gsend[dest] = jnp.concatenate([piece, jnp.full((8 - n_exp, LANES), -1.0, F32)], axis=0)
        gmsg[own_pos, core] = gsend[me]
        for delta in deltas:
            for other in (0, 1):
                if delta == 0 and other == 0:
                    continue
                gate_copy(delta, other).start()

    for chunk in (0, 1):
        for which in range(d_per):
            d_copy(jnp.int32(chunk), which).start()

    def shared_step(step, carry):
        slot = w_pair(step)
        for copy in w_copies_shared(step):
            copy.wait()
        x_own = xbuf[pl.ds(pl.multiple_of(own_row, tok), tok), :]
        both = jnp.dot(x_own, wbuf[slot], preferred_element_type=F32)
        act = (jax.nn.silu(both[:, :LANES]) * both[:, LANES:]).astype(BF16)
        shid[:, pl.ds(pl.multiple_of(step * LANES, LANES), LANES)] = act
        w_start(step + STREAM_SLOTS)
        return carry

    cut_a = sh_steps * 2 // 5
    cut_b = sh_steps * 9 // 10
    with jax.named_scope("shared_a"):
        lax.fori_loop(0, cut_a, shared_step, 0)
    with jax.named_scope("relay_1_0"):
        relay(1, 0)
    with jax.named_scope("shared_b"):
        lax.fori_loop(cut_a, cut_b, shared_step, 0)
    with jax.named_scope("relay_1_1"):
        relay(1, 1)
    with jax.named_scope("shared_c"):
        lax.fori_loop(cut_b, sh_steps, shared_step, 0)

    for delta in deltas:
        for other in (0, 1):
            if delta == 0 and other == 0:
                continue
            if delta == 0:
                src_pos, src_core = own_pos, 1 - core
            else:
                src_pos = pos_at(delta)
                src_core = core if other == 0 else 1 - core
            pltpu.make_async_remote_copy(
                src_ref=gsend.at[0],
                dst_ref=gmsg.at[src_pos, src_core],
                send_sem=g_send.at[src_pos, other],
                recv_sem=g_recv.at[src_pos, src_core],
                device_id={"ep": partner},
                device_id_type=MESH,
            ).wait_recv()

    lane = lax.broadcasted_iota(jnp.int32, (8, LANES), 1)
    packed = []
    for g in range(n_groups):
        b0, b1, b2, b3 = gmsg[2 * g, 0], gmsg[2 * g, 1], gmsg[2 * g + 1, 0], gmsg[2 * g + 1, 1]
        r1 = pltpu.roll(b1, 96, 1)
        r2 = pltpu.roll(b2, 64, 1)
        r3 = pltpu.roll(b3, 32, 1)
        packed.append(jnp.where(lane < 96, b0, r1))
        packed.append(jnp.where(lane < 64, r1, r2))
        packed.append(jnp.where(lane < 32, r2, r3))
    n_tiles = len(packed)
    member = jnp.concatenate([jnp.where(p < 0, 0.0, 1.0) for p in packed], axis=0)
    upper = jnp.where(
        lax.broadcasted_iota(jnp.int32, (LANES, LANES), 0) < lax.broadcasted_iota(jnp.int32, (LANES, LANES), 1), 1.0, 0.0
    ).astype(BF16)
    within = jnp.dot(member.astype(BF16), upper, preferred_element_type=F32)
    base = jnp.zeros((8, 1), F32)
    for t in range(n_tiles):
        m = member[t * 8 : (t + 1) * 8]
        rank = jnp.where(m > 0, within[t * 8 : (t + 1) * 8] + base, -1.0)
        base = base + jnp.sum(m, axis=1, keepdims=True)
        rank_ref[t] = rank
        both = jnp.concatenate([rank, packed[t], jnp.zeros((LANES - 16, LANES), F32)], axis=0)
        cols_ref[t * LANES : (t + 1) * LANES, :] = jnp.transpose(both)

    slot_rows = lax.broadcasted_iota(jnp.int32, (cap, LANES), 0).astype(F32)
    slot_lanes = lax.broadcasted_iota(jnp.int32, (LANES, cap), 1).astype(F32)

    def build(t, carry):
        rank = rank_ref[t]
        col = cols_ref[pl.ds(pl.multiple_of(t * LANES, LANES), LANES), :]
        for e in range(n_exp):
            hot = jnp.where(slot_rows == rank[e : e + 1, :], 1.0, 0.0)
            pick[e * cap : (e + 1) * cap, pl.ds(pl.multiple_of(t * LANES, LANES), LANES)] = hot.astype(BF16)
            hot_t = jnp.where(slot_lanes == col[:, e : e + 1], 1.0, 0.0)
            place[pl.ds(pl.multiple_of(t * LANES, LANES), LANES), e * cap : (e + 1) * cap] = hot_t.astype(BF16)
        return carry

    with jax.named_scope("build"):
        lax.fori_loop(0, n_tiles, build, 0)

    def gather_rows(lo, hi, begin, end):
        def body(n, carry):
            cols = pl.ds(pl.multiple_of(n * 2 * COLS, 2 * COLS), 2 * COLS)
            rows = xbuf[lo:hi, cols]
            for e in range(n_exp):
                got = jnp.dot(pick[e * cap : (e + 1) * cap, lo:hi], rows, preferred_element_type=F32).astype(BF16)
                if lo > 0:
                    got = got + xg[e * cap : (e + 1) * cap, cols]
                xg[e * cap : (e + 1) * cap, cols] = got
            return carry

        lax.fori_loop(begin, end, body, 0)

    def wait_from_core(hops):
        for way in (0, 1):
            if hops == 0 and way == 1:
                continue
            for u in (0, 1) if hops == 0 else halves(way, hops):
                cc_copy(way, hops, u, 1 - core).wait_recv()

    def rows_within(hops):
        return (2 * tok * (1 + 2 * hops)) // LANES * LANES if hops < far else chips * 2 * tok

    wide = n_chunks // 2
    mid = wide // 2
    with jax.named_scope("relay_2_0"):
        relay(2, 0)
        wait_from_core(0)
        wait_from_core(1)
    with jax.named_scope("gather_1"):
        gather_rows(0, rows_within(1), 0, mid)
    with jax.named_scope("relay_2_1"):
        relay(2, 1)
    with jax.named_scope("gather_1"):
        gather_rows(0, rows_within(1), mid, wide)
    with jax.named_scope("wait_2"):
        wait_from_core(2)
    with jax.named_scope("gather_2"):
        gather_rows(rows_within(1), rows_within(2), 0, mid)
    with jax.named_scope("relay_3_0"):
        relay(3, 0)
    with jax.named_scope("gather_2"):
        gather_rows(rows_within(1), rows_within(2), mid, wide)
    with jax.named_scope("relay_3_1"):
        relay(3, 1)
    with jax.named_scope("wait_3"):
        wait_from_core(3)
    with jax.named_scope("gather_3"):
        gather_rows(rows_within(2), rows_within(3), 0, mid)
    with jax.named_scope("relay_4_0"):
        relay(4, 0)
    with jax.named_scope("gather_3"):
        gather_rows(rows_within(2), rows_within(3), mid, wide)
    with jax.named_scope("wait_4"):
        wait_from_core(4)
    with jax.named_scope("gather_4"):
        gather_rows(rows_within(3), rows_within(4), 0, wide)

    def up_expert(exp, carry):
        rows = pl.ds(pl.multiple_of(exp * cap, cap), cap)
        first = sh_steps + exp * ex_steps
        for lo in range(0, ex_steps, STEP_UNITS):
            units = range(lo, min(lo + STEP_UNITS, ex_steps))
            for j in units:
                for copy in w_copies_expert(first + j):
                    copy.wait()
            for j in units:
                both = jnp.dot(xg[rows, :], wbuf[w_pair(first + j)], preferred_element_type=F32)
                act = (jax.nn.silu(both[:, :LANES]) * both[:, LANES:]).astype(BF16)
                hid[rows, j * LANES : (j + 1) * LANES] = act
            for j in units:
                w_start(first + j + STREAM_SLOTS)
        return carry

    with jax.named_scope("up"):
        lax.fori_loop(0, n_exp, up_expert, 0)

    def part_copy(chunk):
        par = lax.rem(chunk, 2)
        return pltpu.make_async_remote_copy(
            src_ref=part.at[par, :, 1 - core],
            dst_ref=from_core.at[chunk],
            send_sem=p_send.at[chunk],
            recv_sem=p_recv.at[chunk],
            device_id={"ep": partner},
            device_id_type=MESH,
        )

    def ring_copy(chunk, way, hop):
        dev = {"ep": at_chip(1 if way == 0 else -1, core)}
        if hop == 1:
            src = from_core.at[chunk, far_pos, pl.ds(way * half, half), :]
            dst = ring.at[chunk, way, 0, pl.ds(way * half, half), :]
        else:
            src = ring.at[chunk, way, hop - 2]
            dst = ring.at[chunk, way, hop - 1]
        return pltpu.make_async_remote_copy(
            src_ref=src,
            dst_ref=dst,
            send_sem=r_send.at[chunk, way, hop - 1],
            recv_sem=r_recv.at[chunk, way, hop - 1],
            device_id=dev,
            device_id_type=MESH,
        )

    def dest_pos(way, hops):
        return pos_of(1 - way, hops)

    def compute(chunk):
        par = lax.rem(chunk, 2)
        cols = pl.ds(pl.multiple_of(chunk * COLS, COLS), COLS)
        for which in range(d_per):
            d_copy(chunk, which).wait()

        @pl.when(chunk >= 2)
        def _():
            part_copy(chunk - 2).wait_send()

        for e in range(n_exp):
            got = jnp.dot(hid[e * cap : (e + 1) * cap, :], dbuf[par * d_per + e], preferred_element_type=F32)
            erows[e * cap : (e + 1) * cap, :] = got.astype(BF16)
        shared = jnp.dot(shid[:, :inter], dbuf[par * d_per + n_exp], preferred_element_type=F32)
        shared = shared + jnp.dot(shid[:, inter:], dbuf[par * d_per + n_exp + 1], preferred_element_type=F32)
        sout[:, cols] = shared.astype(BF16)
        for g in range(n_groups):
            rows = slice(g * group_rows, (g + 1) * group_rows)
            acc = None
            for e in range(n_exp):
                got = jnp.dot(
                    place[rows, e * cap : (e + 1) * cap], erows[e * cap : (e + 1) * cap, :], preferred_element_type=F32
                )
                got = cols_ref[rows, 8 + e : 9 + e] * got
                acc = got if acc is None else acc + got
            for b in range(4):
                part[par, 2 * g + b // 2, b % 2] = acc[b * tok : (b + 1) * tok]

        @pl.when(chunk + 2 < n_chunks)
        def _():
            for which in range(d_per):
                d_copy(chunk + 2, which).start()

        part_copy(chunk).start()

    def fold(chunk):
        par = lax.rem(chunk, 2)
        part_copy(chunk).wait_recv()
        for pos in range(chips):
            from_core[chunk, pos] = from_core[chunk, pos] + part[par, pos, core]
        for way in (0, 1):
            ring_copy(chunk, way, 1).start()

    def pass_on(chunk, hop):
        for way in (0, 1):
            ring_copy(chunk, way, hop).wait_recv()
            pos = dest_pos(way, far - hop)
            if hop == 1:
                done = pl.ds(way * half, half)
                rest = pl.ds((1 - way) * half, half)
                ring[chunk, way, 0, done, :] = ring[chunk, way, 0, done, :] + from_core[chunk, pos, done, :]
                ring[chunk, way, 0, rest, :] = from_core[chunk, pos, rest, :]
            else:
                ring[chunk, way, hop - 1] = ring[chunk, way, hop - 1] + from_core[chunk, pos]
            ring_copy(chunk, way, hop + 1).start()

    def finish(chunk):
        cols = pl.ds(pl.multiple_of(chunk * COLS, COLS), COLS)
        for way in (0, 1):
            ring_copy(chunk, way, far).wait_recv()
        routed = from_core[chunk, own_pos] + ring[chunk, 0, far - 1] + ring[chunk, 1, far - 1]
        out_ref[:, cols] = (hidden_ref[:, cols].astype(F32) + sout[:, cols].astype(F32) + routed).astype(BF16)

    def turn(i, carry):
        @pl.when(i < n_chunks)
        def _():
            with jax.named_scope("compute"):
                compute(i)

        @pl.when((i >= far) & (i - far < n_chunks))
        def _():
            with jax.named_scope("finish"):
                finish(i - far)

        for hop in range(far - 1, 0, -1):
            @pl.when((i >= hop) & (i - hop < n_chunks))
            def _():
                with jax.named_scope("pass_on"):
                    pass_on(i - hop, hop)

        @pl.when(i < n_chunks)
        def _():
            with jax.named_scope("fold"):
                fold(i)

        return carry

    lax.fori_loop(0, n_chunks + far, turn, 0)

    for hops in range(1, far + 1):
        for way in (0, 1):
            for u in halves(way, hops):
                ag_copy(way, hops, u).wait_send()
                cc_copy(way, hops, u, core).wait_send()
    for u in (0, 1):
        cc_copy(0, 0, u, core).wait_send()
    for delta in deltas:
        for other in (0, 1):
            if not (delta == 0 and other == 0):
                gate_copy(delta, other).wait_send()

    def drain(chunk, carry):
        @pl.when(chunk >= n_chunks - 2)
        def _():
            part_copy(chunk).wait_send()

        for way in (0, 1):
            for hop in range(1, far + 1):
                ring_copy(chunk, way, hop).wait_send()
        return carry

    lax.fori_loop(0, n_chunks, drain, 0)


def solution(mesh):
    ep_size = mesh.shape["ep"]

    def local_block(hidden_in, norm_gain, router_w, w_gate, w_up, w_down, ws_gate, ws_up, ws_down, expert_ids):
        tok, top_k = expert_ids.shape
        dim = hidden_in.shape[1]
        n_exp, _, inter = w_gate.shape
        s_inter = ws_gate.shape[1]
        chips = ep_size // 2
        far = chips // 2
        n_chunks = dim // COLS
        pair_cap = GROUPS * ((top_k + GROUP_LIMIT - 1) // GROUP_LIMIT) * tok // ep_size
        cap = pair_cap * ep_size // n_exp
        all_tok = ep_size * tok
        slots = n_exp * cap
        n_tiles = all_tok // LANES
        vmem = pl.BlockSpec(memory_space=pltpu.VMEM)
        hbm = pl.BlockSpec(memory_space=pl.ANY)
        dma = pltpu.SemaphoreType.DMA
        return pl.pallas_call(
            functools.partial(moe_kernel, ep_size, cap),
            out_shape=jax.ShapeDtypeStruct((tok, dim), BF16),
            in_specs=[vmem] * 4 + [hbm] * 6,
            out_specs=vmem,
            scratch_shapes=[
                pltpu.VMEM((all_tok, dim), BF16),
                pltpu.VMEM((ep_size, 8, LANES), F32),
                pltpu.VMEM((chips, 2, 8, LANES), F32),
                pltpu.VMEM((n_tiles, 8, LANES), F32),
                pltpu.VMEM((all_tok, LANES), F32),
                pltpu.VMEM((slots, all_tok), BF16),
                pltpu.VMEM((all_tok, slots), BF16),
                pltpu.VMEM((slots, dim), BF16),
                pltpu.VMEM((slots, inter), BF16),
                pltpu.VMEM((tok, s_inter), BF16),
                pltpu.VMEM((tok, dim), BF16),
                pltpu.VMEM((STREAM_SLOTS, dim, 2 * LANES), BF16),
                pltpu.VMEM((2 * (n_exp + 2), inter, COLS), BF16),
                pltpu.VMEM((2, chips, 2, tok, COLS), F32),
                pltpu.VMEM((slots, COLS), BF16),
                pltpu.VMEM((n_chunks, chips, tok, COLS), F32),
                pltpu.VMEM((n_chunks, 2, far, tok, COLS), F32),
                dma((STREAM_SLOTS, 2)),
                dma((2 * (n_exp + 2),)),
                dma((2, far, 2)),
                dma((2, far, 2)),
                dma((2, far + 1, 2)),
                dma((2, far + 1, 2)),
                dma((chips, 2)),
                dma((chips, 2)),
                dma((n_chunks,)),
                dma((n_chunks,)),
                dma((n_chunks, 2, far)),
                dma((n_chunks, 2, far)),
            ],
            compiler_params=pltpu.CompilerParams(
                collective_id=0, has_side_effects=True, vmem_limit_bytes=67043328
            ),
        )(hidden_in, norm_gain.reshape(1, dim), router_w, expert_ids.T, w_gate, w_up, w_down, ws_gate, ws_up, ws_down)

    row_spec = P(("dp", "ep"), None)
    in_specs = (row_spec, P(), P(), P("ep"), P("ep"), P("ep"), P(), P(), P(), row_spec)
    return jax.shard_map(local_block, mesh=mesh, in_specs=in_specs, out_specs=row_spec, check_vma=False)
```

```python
import functools

import jax
import jax.numpy as jnp
from jax import lax
from jax.experimental import pallas as pl
from jax.experimental.pallas import tpu as pltpu
from jax.sharding import PartitionSpec as P

NORM_EPS = 1e-6
ROUTE_SCALE = 2.5
GROUPS = 8
GROUP_LIMIT = 4
LANES = 128
COLS = 256
STREAM_SLOTS = 8
STEP_UNITS = 4
MESH = pl.DeviceIdType.MESH
F32 = jnp.float32
BF16 = jnp.bfloat16


def moe_kernel(
    ep_size,
    cap,
    hidden_hbm,
    gain_hbm,
    router_hbm,
    ids_hbm,
    wg_hbm,
    wu_hbm,
    wd_hbm,
    sg_hbm,
    su_hbm,
    sd_hbm,
    out_ref,
    xbuf,
    gsend,
    gmsg,
    rank_ref,
    cols_ref,
    pick,
    place,
    xg,
    hid,
    shid,
    sout,
    wbuf,
    dbuf,
    part,
    erows,
    from_core,
    ring,
    w_sem,
    d_sem,
    ag_send,
    ag_recv,
    cc_send,
    cc_recv,
    g_send,
    g_recv,
    p_send,
    p_recv,
    r_send,
    r_recv,
    hidden_ref,
    gain_ref,
    router_ref,
    ids_ref,
    i_sem,
):
    tok, dim = hidden_hbm.shape
    half = tok // 2
    top_k = ids_hbm.shape[0]
    n_exp = wg_hbm.shape[0]
    inter = wg_hbm.shape[2]
    s_inter = sg_hbm.shape[1]
    chips = ep_size // 2
    far = chips // 2
    own_pos = 0
    far_pos = chips - 1
    n_groups = chips // 2
    group_rows = 4 * tok
    tiles_per_group = group_rows // LANES
    n_chunks = dim // COLS
    slots = n_exp * cap
    sh_steps = s_inter // LANES
    ex_steps = inter // LANES
    w_steps = sh_steps + n_exp * ex_steps
    d_per = n_exp + 2

    me = lax.axis_index("ep")
    core = lax.rem(me, 2)
    chip = me // 2
    partner = chip * 2 + (1 - core)

    def at_chip(delta, which):
        return lax.rem(chip + delta + chips, chips) * 2 + which

    def pos_of(way, hops):
        return far_pos if hops == far else 2 * hops - 1 + way

    def pos_at(delta):
        if delta == 0:
            return own_pos
        if abs(delta) == far:
            return far_pos
        return pos_of(0, delta) if delta > 0 else pos_of(1, -delta)

    def row_at(pos, which):
        return pos * 2 * tok + which * tok

    def w_pair(step):
        slot = lax.rem(step, STREAM_SLOTS)
        return slot

    def w_copies_shared(step):
        slot = w_pair(step)
        col = pl.ds(pl.multiple_of(step * LANES, LANES), LANES)
        return (
            pltpu.make_async_copy(sg_hbm.at[:, col], wbuf.at[slot, :, pl.ds(0, LANES)], w_sem.at[slot, 0]),
            pltpu.make_async_copy(su_hbm.at[:, col], wbuf.at[slot, :, pl.ds(LANES, LANES)], w_sem.at[slot, 1]),
        )

    def w_copies_expert(step):
        slot = w_pair(step)
        rel = step - sh_steps
        exp = rel // ex_steps
        col = pl.ds(pl.multiple_of((rel - exp * ex_steps) * LANES, LANES), LANES)
        return (
            pltpu.make_async_copy(wg_hbm.at[exp, :, col], wbuf.at[slot, :, pl.ds(0, LANES)], w_sem.at[slot, 0]),
            pltpu.make_async_copy(wu_hbm.at[exp, :, col], wbuf.at[slot, :, pl.ds(LANES, LANES)], w_sem.at[slot, 1]),
        )

    def w_start(step):
        @pl.when(step < sh_steps)
        def _():
            for copy in w_copies_shared(step):
                copy.start()

        @pl.when((step >= sh_steps) & (step < w_steps))
        def _():
            for copy in w_copies_expert(step):
                copy.start()

    def d_copy(chunk, which):
        slot = lax.rem(chunk, 2) * d_per + which
        col = pl.ds(pl.multiple_of(chunk * COLS, COLS), COLS)
        if which < n_exp:
            src = wd_hbm.at[which, :, col]
        else:
            src = sd_hbm.at[pl.ds((which - n_exp) * inter, inter), col]
        return pltpu.make_async_copy(src, dbuf.at[slot], d_sem.at[slot])

    def ag_copy(way, hops, u):
        src_row = row_at(own_pos if hops == 1 else pos_of(way, hops - 1), core) + u * half
        dst_row = row_at(pos_of(way, hops), core) + u * half
        return pltpu.make_async_remote_copy(
            src_ref=xbuf.at[pl.ds(src_row, half), :],
            dst_ref=xbuf.at[pl.ds(dst_row, half), :],
            send_sem=ag_send.at[way, hops - 1, u],
            recv_sem=ag_recv.at[way, hops - 1, u],
            device_id={"ep": at_chip(1 if way == 0 else -1, core)},
            device_id_type=MESH,
        )

    def cc_copy(way, hops, u, which):
        pos = own_pos if hops == 0 else pos_of(way, hops)
        rows = pl.ds(row_at(pos, which) + u * half, half)
        return pltpu.make_async_remote_copy(
            src_ref=xbuf.at[rows, :],
            dst_ref=xbuf.at[rows, :],
            send_sem=cc_send.at[way, hops, u],
            recv_sem=cc_recv.at[way, hops, u],
            device_id={"ep": partner},
            device_id_type=MESH,
        )

    def halves(way, hops):
        if hops == far:
            return (way,)
        return (0, 1) if way == 0 else (1, 0)

    def relay(hops, nth):
        for way in (0, 1):
            if nth >= len(halves(way, hops)):
                continue
            u = halves(way, hops)[nth]
            ag_copy(way, hops, u).wait_recv()
            if hops < far and u in halves(way, hops + 1):
                ag_copy(way, hops + 1, u).start()
            cc_copy(way, hops, u, core).start()

    def gate_copy(delta, other):
        dst_pos = pos_at(delta)
        dest = partner if delta == 0 else at_chip(delta, core if other == 0 else 1 - core)
        return pltpu.make_async_remote_copy(
            src_ref=gsend.at[dest],
            dst_ref=gmsg.at[dst_pos, core],
            send_sem=g_send.at[dst_pos, other],
            recv_sem=g_recv.at[dst_pos, core],
            device_id={"ep": dest},
            device_id_type=MESH,
        )

    deltas = [d for d in range(-(far - 1), far + 1)]

    barrier = pltpu.get_barrier_semaphore()
    for off in range(1, ep_size):
        pl.semaphore_signal(barrier, inc=1, device_id={"ep": lax.rem(me + off, ep_size)}, device_id_type=MESH)
    small = [
        pltpu.make_async_copy(src, dst, i_sem.at[k])
        for k, (src, dst) in enumerate(
            ((hidden_hbm, hidden_ref), (gain_hbm, gain_ref), (ids_hbm, ids_ref), (router_hbm, router_ref))
        )
    ]
    for copy in small:
        copy.start()
    small[0].wait()
    small[1].wait()

    x_f32 = hidden_ref[...].astype(F32)
    inv_rms = lax.rsqrt(jnp.mean(x_f32 * x_f32, axis=-1, keepdims=True) + NORM_EPS)
    x_norm = (x_f32 * inv_rms * gain_ref[...]).astype(BF16)
    own_row = row_at(own_pos, core)
    xbuf[pl.ds(pl.multiple_of(own_row, tok), tok), :] = x_norm

    with jax.named_scope("barrier"):
        pl.semaphore_wait(barrier, ep_size - 1)
    for nth in (0, 1):
        for way in (0, 1):
            ag_copy(way, 1, halves(way, 1)[nth]).start()
    for u in (0, 1):
        cc_copy(0, 0, u, core).start()
    for step in range(STREAM_SLOTS):
        w_start(jnp.int32(step))

    with jax.named_scope("gates"):
        small[2].wait()
        small[3].wait()
        logits = lax.dot_general(
            router_ref[...],
            x_norm.astype(F32),
            (((1,), (1,)), ((), ())),
            precision=lax.Precision.HIGHEST,
            preferred_element_type=F32,
        )
        scores = jax.nn.sigmoid(logits)
        exp_iota = lax.broadcasted_iota(jnp.int32, scores.shape, 0)
        chosen = exp_iota == ids_ref[0:1, :]
        for k in range(1, top_k):
            chosen = chosen | (exp_iota == ids_ref[k : k + 1, :])
        total = jnp.sum(jnp.where(chosen, scores, 0.0), axis=0, keepdims=True)
        gates = jnp.where(chosen, ROUTE_SCALE * scores / total, -1.0)
        gates_t = jnp.concatenate([gates, jnp.full((gates.shape[0], LANES - tok), -1.0, F32)], axis=1)
        for dest in range(ep_size):
            piece = gates_t[dest * n_exp : (dest + 1) * n_exp, :]
            gsend[dest] = jnp.concatenate([piece, jnp.full((8 - n_exp, LANES), -1.0, F32)], axis=0)
        gmsg[own_pos, core] = gsend[me]
        for delta in deltas:
            for other in (0, 1):
                if delta == 0 and other == 0:
                    continue
                gate_copy(delta, other).start()

    for chunk in (0, 1):
        for which in range(d_per):
            d_copy(jnp.int32(chunk), which).start()

    def shared_step(step, carry):
        slot = w_pair(step)
        for copy in w_copies_shared(step):
            copy.wait()
        x_own = xbuf[pl.ds(pl.multiple_of(own_row, tok), tok), :]
        both = jnp.dot(x_own, wbuf[slot], preferred_element_type=F32)
        act = (jax.nn.silu(both[:, :LANES]) * both[:, LANES:]).astype(BF16)
        shid[:, pl.ds(pl.multiple_of(step * LANES, LANES), LANES)] = act
        w_start(step + STREAM_SLOTS)
        return carry

    cut_a = sh_steps * 2 // 5
    cut_b = sh_steps * 9 // 10
    with jax.named_scope("shared_a"):
        lax.fori_loop(0, cut_a, shared_step, 0)
    with jax.named_scope("relay_1_0"):
        relay(1, 0)
    with jax.named_scope("shared_b"):
        lax.fori_loop(cut_a, cut_b, shared_step, 0)
    with jax.named_scope("relay_1_1"):
        relay(1, 1)
    with jax.named_scope("shared_c"):
        lax.fori_loop(cut_b, sh_steps, shared_step, 0)

    for delta in deltas:
        for other in (0, 1):
            if delta == 0 and other == 0:
                continue
            if delta == 0:
                src_pos, src_core = own_pos, 1 - core
            else:
                src_pos = pos_at(delta)
                src_core = core if other == 0 else 1 - core
            pltpu.make_async_remote_copy(
                src_ref=gsend.at[0],
                dst_ref=gmsg.at[src_pos, src_core],
                send_sem=g_send.at[src_pos, other],
                recv_sem=g_recv.at[src_pos, src_core],
                device_id={"ep": partner},
                device_id_type=MESH,
            ).wait_recv()

    lane = lax.broadcasted_iota(jnp.int32, (8, LANES), 1)
    packed = []
    for g in range(n_groups):
        b0, b1, b2, b3 = gmsg[2 * g, 0], gmsg[2 * g, 1], gmsg[2 * g + 1, 0], gmsg[2 * g + 1, 1]
        r1 = pltpu.roll(b1, 96, 1)
        r2 = pltpu.roll(b2, 64, 1)
        r3 = pltpu.roll(b3, 32, 1)
        packed.append(jnp.where(lane < 96, b0, r1))
        packed.append(jnp.where(lane < 64, r1, r2))
        packed.append(jnp.where(lane < 32, r2, r3))
    n_tiles = len(packed)
    member = jnp.concatenate([jnp.where(p < 0, 0.0, 1.0) for p in packed], axis=0)
    upper = jnp.where(
        lax.broadcasted_iota(jnp.int32, (LANES, LANES), 0) < lax.broadcasted_iota(jnp.int32, (LANES, LANES), 1), 1.0, 0.0
    ).astype(BF16)
    within = jnp.dot(member.astype(BF16), upper, preferred_element_type=F32)
    base = jnp.zeros((8, 1), F32)
    for t in range(n_tiles):
        m = member[t * 8 : (t + 1) * 8]
        rank = jnp.where(m > 0, within[t * 8 : (t + 1) * 8] + base, -1.0)
        base = base + jnp.sum(m, axis=1, keepdims=True)
        rank_ref[t] = rank
        both = jnp.concatenate([rank, packed[t], jnp.zeros((LANES - 16, LANES), F32)], axis=0)
        cols_ref[t * LANES : (t + 1) * LANES, :] = jnp.transpose(both)

    slot_rows = lax.broadcasted_iota(jnp.int32, (cap, LANES), 0).astype(F32)
    slot_lanes = lax.broadcasted_iota(jnp.int32, (LANES, cap), 1).astype(F32)

    def build(t, carry):
        rank = rank_ref[t]
        col = cols_ref[pl.ds(pl.multiple_of(t * LANES, LANES), LANES), :]
        for e in range(n_exp):
            hot = jnp.where(slot_rows == rank[e : e + 1, :], 1.0, 0.0)
            pick[e * cap : (e + 1) * cap, pl.ds(pl.multiple_of(t * LANES, LANES), LANES)] = hot.astype(BF16)
            hot_t = jnp.where(slot_lanes == col[:, e : e + 1], 1.0, 0.0)
            place[pl.ds(pl.multiple_of(t * LANES, LANES), LANES), e * cap : (e + 1) * cap] = hot_t.astype(BF16)
        return carry

    with jax.named_scope("build"):
        lax.fori_loop(0, n_tiles, build, 0)

    def gather_rows(lo, hi, begin, end):
        def body(n, carry):
            cols = pl.ds(pl.multiple_of(n * 2 * COLS, 2 * COLS), 2 * COLS)
            rows = xbuf[lo:hi, cols]
            for e in range(n_exp):
                got = jnp.dot(pick[e * cap : (e + 1) * cap, lo:hi], rows, preferred_element_type=F32).astype(BF16)
                if lo > 0:
                    got = got + xg[e * cap : (e + 1) * cap, cols]
                xg[e * cap : (e + 1) * cap, cols] = got
            return carry

        lax.fori_loop(begin, end, body, 0)

    def wait_from_core(hops):
        for way in (0, 1):
            if hops == 0 and way == 1:
                continue
            for u in (0, 1) if hops == 0 else halves(way, hops):
                cc_copy(way, hops, u, 1 - core).wait_recv()

    def rows_within(hops):
        return (2 * tok * (1 + 2 * hops)) // LANES * LANES if hops < far else chips * 2 * tok

    wide = n_chunks // 2
    mid = wide // 2
    with jax.named_scope("relay_2_0"):
        relay(2, 0)
        wait_from_core(0)
        wait_from_core(1)
    with jax.named_scope("gather_1"):
        gather_rows(0, rows_within(1), 0, mid)
    with jax.named_scope("relay_2_1"):
        relay(2, 1)
    with jax.named_scope("gather_1"):
        gather_rows(0, rows_within(1), mid, wide)
    with jax.named_scope("wait_2"):
        wait_from_core(2)
    with jax.named_scope("gather_2"):
        gather_rows(rows_within(1), rows_within(2), 0, mid)
    with jax.named_scope("relay_3_0"):
        relay(3, 0)
    with jax.named_scope("gather_2"):
        gather_rows(rows_within(1), rows_within(2), mid, wide)
    with jax.named_scope("relay_3_1"):
        relay(3, 1)
    with jax.named_scope("wait_3"):
        wait_from_core(3)
    with jax.named_scope("gather_3"):
        gather_rows(rows_within(2), rows_within(3), 0, mid)
    with jax.named_scope("relay_4_0"):
        relay(4, 0)
    with jax.named_scope("gather_3"):
        gather_rows(rows_within(2), rows_within(3), mid, wide)
    with jax.named_scope("wait_4"):
        wait_from_core(4)
    with jax.named_scope("gather_4"):
        gather_rows(rows_within(3), rows_within(4), 0, wide)

    def up_expert(exp, carry):
        rows = pl.ds(pl.multiple_of(exp * cap, cap), cap)
        first = sh_steps + exp * ex_steps
        for lo in range(0, ex_steps, STEP_UNITS):
            units = range(lo, min(lo + STEP_UNITS, ex_steps))
            for j in units:
                for copy in w_copies_expert(first + j):
                    copy.wait()
            for j in units:
                both = jnp.dot(xg[rows, :], wbuf[w_pair(first + j)], preferred_element_type=F32)
                act = (jax.nn.silu(both[:, :LANES]) * both[:, LANES:]).astype(BF16)
                hid[rows, j * LANES : (j + 1) * LANES] = act
            for j in units:
                w_start(first + j + STREAM_SLOTS)
        return carry

    with jax.named_scope("up"):
        lax.fori_loop(0, n_exp, up_expert, 0)

    def part_copy(chunk, rest):
        par = lax.rem(chunk, 2)
        which = pl.ds(0, far_pos) if rest else pl.ds(far_pos, 1)
        return pltpu.make_async_remote_copy(
            src_ref=part.at[par, which, 1 - core],
            dst_ref=from_core.at[chunk, which],
            send_sem=p_send.at[chunk, rest],
            recv_sem=p_recv.at[chunk, rest],
            device_id={"ep": partner},
            device_id_type=MESH,
        )

    def ring_copy(chunk, way, hop):
        dev = {"ep": at_chip(1 if way == 0 else -1, core)}
        if hop == 1:
            src = from_core.at[chunk, far_pos, pl.ds(way * half, half), :]
            dst = ring.at[chunk, way, 0, pl.ds(way * half, half), :]
        else:
            src = ring.at[chunk, way, hop - 2]
            dst = ring.at[chunk, way, hop - 1]
        return pltpu.make_async_remote_copy(
            src_ref=src,
            dst_ref=dst,
            send_sem=r_send.at[chunk, way, hop - 1],
            recv_sem=r_recv.at[chunk, way, hop - 1],
            device_id=dev,
            device_id_type=MESH,
        )

    def dest_pos(way, hops):
        return pos_of(1 - way, hops)

    def down(chunk):
        par = lax.rem(chunk, 2)
        for which in range(d_per):
            d_copy(chunk, which).wait()
        for e in range(n_exp):
            got = jnp.dot(hid[e * cap : (e + 1) * cap, :], dbuf[par * d_per + e], preferred_element_type=F32)
            erows[e * cap : (e + 1) * cap, :] = got.astype(BF16)
        shared = jnp.dot(shid[:, :inter], dbuf[par * d_per + n_exp], preferred_element_type=F32)
        shared = shared + jnp.dot(shid[:, inter:], dbuf[par * d_per + n_exp + 1], preferred_element_type=F32)
        sout[:, pl.ds(pl.multiple_of(chunk * COLS, COLS), COLS)] = shared.astype(BF16)

        @pl.when(chunk + 2 < n_chunks)
        def _():
            for which in range(d_per):
                d_copy(chunk + 2, which).start()

    def combine(chunk, groups):
        par = lax.rem(chunk, 2)
        for g in groups:
            rows = slice(g * group_rows, (g + 1) * group_rows)
            acc = None
            for e in range(n_exp):
                got = jnp.dot(
                    place[rows, e * cap : (e + 1) * cap], erows[e * cap : (e + 1) * cap, :], preferred_element_type=F32
                )
                got = cols_ref[rows, 8 + e : 9 + e] * got
                acc = got if acc is None else acc + got
            for b in range(4):
                part[par, 2 * g + b // 2, b % 2] = acc[b * tok : (b + 1) * tok]

    def fold_rest(chunk):
        par = lax.rem(chunk, 2)
        part_copy(chunk, 1).wait_recv()
        for pos in range(far_pos):
            from_core[chunk, pos] = from_core[chunk, pos] + part[par, pos, core]

    def first_hop(chunk):
        par = lax.rem(chunk, 2)
        part_copy(chunk, 0).wait_recv()
        from_core[chunk, far_pos] = from_core[chunk, far_pos] + part[par, far_pos, core]
        for way in (0, 1):
            ring_copy(chunk, way, 1).start()

    def pass_on(chunk, hop):
        for way in (0, 1):
            ring_copy(chunk, way, hop).wait_recv()
            pos = dest_pos(way, far - hop)
            if hop == 1:
                done = pl.ds(way * half, half)
                rest = pl.ds((1 - way) * half, half)
                ring[chunk, way, 0, done, :] = ring[chunk, way, 0, done, :] + from_core[chunk, pos, done, :]
                ring[chunk, way, 0, rest, :] = from_core[chunk, pos, rest, :]
            else:
                ring[chunk, way, hop - 1] = ring[chunk, way, hop - 1] + from_core[chunk, pos]
            ring_copy(chunk, way, hop + 1).start()

    def finish(chunk):
        cols = pl.ds(pl.multiple_of(chunk * COLS, COLS), COLS)
        for way in (0, 1):
            ring_copy(chunk, way, far).wait_recv()
        routed = from_core[chunk, own_pos] + ring[chunk, 0, far - 1] + ring[chunk, 1, far - 1]
        out_ref[:, cols] = (hidden_ref[:, cols].astype(F32) + sout[:, cols].astype(F32) + routed).astype(BF16)

        @pl.when(chunk >= 1)
        def _():
            ring_sends_done(chunk - 1)

    def ring_sends_done(chunk):
        for way in (0, 1):
            for hop in range(1, far + 1):
                ring_copy(chunk, way, hop).wait_send()

    def gather_sends_done():
        for hops in range(1, far + 1):
            for way in (0, 1):
                for u in halves(way, hops):
                    ag_copy(way, hops, u).wait_send()
                    cc_copy(way, hops, u, core).wait_send()
        for u in (0, 1):
            cc_copy(0, 0, u, core).wait_send()
        for delta in deltas:
            for other in (0, 1):
                if not (delta == 0 and other == 0):
                    gate_copy(delta, other).wait_send()

    def turn(i, carry):
        def for_chunk(lag, name, fn):
            @pl.when((i >= lag) & (i - lag < n_chunks))
            def _():
                with jax.named_scope(name):
                    fn(i - lag)

        def hops_of(in_middle):
            for hop in range(1, far + 1):
                if (hop % 2 == 0) == in_middle:
                    lag = 3 * hop // 2 if in_middle else (3 * hop - 1) // 2
                    if hop == far:
                        for_chunk(lag, "finish", finish)
                    else:
                        for_chunk(lag, "pass_on", functools.partial(pass_on, hop=hop))

        for_chunk(0, "down", down)
        for_chunk(1, "fold_rest", fold_rest)
        hops_of(True)

        @pl.when(i < n_chunks)
        def _():
            @pl.when(i >= 2)
            def _():
                for rest in (0, 1):
                    part_copy(i - 2, rest).wait_send()

            with jax.named_scope("combine_far"):
                combine(i, (n_groups - 1,))
                part_copy(i, 0).start()
            with jax.named_scope("combine"):
                combine(i, range(n_groups - 1))
                part_copy(i, 1).start()

        for_chunk(0, "first_hop", first_hop)
        hops_of(False)

        @pl.when(i == n_chunks)
        def _():
            gather_sends_done()

        return carry

    lax.fori_loop(0, n_chunks + 3 * far // 2, turn, 0)

    for chunk in (n_chunks - 2, n_chunks - 1):
        for rest in (0, 1):
            part_copy(jnp.int32(chunk), rest).wait_send()
    ring_sends_done(jnp.int32(n_chunks - 1))


def solution(mesh):
    ep_size = mesh.shape["ep"]

    def local_block(hidden_in, norm_gain, router_w, w_gate, w_up, w_down, ws_gate, ws_up, ws_down, expert_ids):
        tok, top_k = expert_ids.shape
        dim = hidden_in.shape[1]
        n_exp, _, inter = w_gate.shape
        s_inter = ws_gate.shape[1]
        chips = ep_size // 2
        far = chips // 2
        n_chunks = dim // COLS
        pair_cap = GROUPS * ((top_k + GROUP_LIMIT - 1) // GROUP_LIMIT) * tok // ep_size
        cap = pair_cap * ep_size // n_exp
        all_tok = ep_size * tok
        slots = n_exp * cap
        n_tiles = all_tok // LANES
        vmem = pl.BlockSpec(memory_space=pltpu.VMEM)
        hbm = pl.BlockSpec(memory_space=pl.ANY)
        dma = pltpu.SemaphoreType.DMA
        return pl.pallas_call(
            functools.partial(moe_kernel, ep_size, cap),
            out_shape=pltpu.VMEM((tok, dim), BF16),
            in_specs=[hbm] * 10,
            out_specs=vmem,
            scratch_shapes=[
                pltpu.VMEM((all_tok, dim), BF16),
                pltpu.VMEM((ep_size, 8, LANES), F32),
                pltpu.VMEM((chips, 2, 8, LANES), F32),
                pltpu.VMEM((n_tiles, 8, LANES), F32),
                pltpu.VMEM((all_tok, LANES), F32),
                pltpu.VMEM((slots, all_tok), BF16),
                pltpu.VMEM((all_tok, slots), BF16),
                pltpu.VMEM((slots, dim), BF16),
                pltpu.VMEM((slots, inter), BF16),
                pltpu.VMEM((tok, s_inter), BF16),
                pltpu.VMEM((tok, dim), BF16),
                pltpu.VMEM((STREAM_SLOTS, dim, 2 * LANES), BF16),
                pltpu.VMEM((2 * (n_exp + 2), inter, COLS), BF16),
                pltpu.VMEM((2, chips, 2, tok, COLS), F32),
                pltpu.VMEM((slots, COLS), BF16),
                pltpu.VMEM((n_chunks, chips, tok, COLS), F32),
                pltpu.VMEM((n_chunks, 2, far, tok, COLS), F32),
                dma((STREAM_SLOTS, 2)),
                dma((2 * (n_exp + 2),)),
                dma((2, far, 2)),
                dma((2, far, 2)),
                dma((2, far + 1, 2)),
                dma((2, far + 1, 2)),
                dma((chips, 2)),
                dma((chips, 2)),
                dma((n_chunks, 2)),
                dma((n_chunks, 2)),
                dma((n_chunks, 2, far)),
                dma((n_chunks, 2, far)),
                pltpu.VMEM((tok, dim), BF16),
                pltpu.VMEM((1, dim), F32),
                pltpu.VMEM(router_w.shape, F32),
                pltpu.VMEM((top_k, tok), jnp.int32),
                dma((4,)),
            ],
            compiler_params=pltpu.CompilerParams(
                collective_id=0, has_side_effects=True, vmem_limit_bytes=66000000
            ),
        )(hidden_in, norm_gain.reshape(1, dim), router_w, expert_ids.T, w_gate, w_up, w_down, ws_gate, ws_up, ws_down)

    row_spec = P(("dp", "ep"), None)
    in_specs = (row_spec, P(), P(), P("ep"), P("ep"), P("ep"), P(), P(), P(), row_spec)
    return jax.shard_map(local_block, mesh=mesh, in_specs=in_specs, out_specs=row_spec, check_vma=False)
```

```python
import functools

import jax
import jax.numpy as jnp
from jax import lax
from jax.experimental import pallas as pl
from jax.experimental.pallas import tpu as pltpu
from jax.sharding import PartitionSpec as P

NORM_EPS = 1e-6
ROUTE_SCALE = 2.5
GROUPS = 8
GROUP_LIMIT = 4
LANES = 128
COLS = 256
STREAM_SLOTS = 16
STEP_UNITS = 6
MESH = pl.DeviceIdType.MESH
F32 = jnp.float32
BF16 = jnp.bfloat16


def moe_kernel(
    ep_size,
    cap,
    hidden_hbm,
    gain_hbm,
    router_hbm,
    ids_hbm,
    wg_hbm,
    wu_hbm,
    wd_hbm,
    sg_hbm,
    su_hbm,
    sd_hbm,
    out_ref,
    xbuf,
    gsend,
    gmsg,
    rank_ref,
    cols_ref,
    pick,
    place,
    xg,
    hid,
    shid,
    sout,
    wbuf,
    dbuf,
    part,
    erows,
    from_core,
    ring,
    w_sem,
    d_sem,
    ag_send,
    ag_recv,
    cc_send,
    cc_recv,
    g_send,
    g_recv,
    p_send,
    p_recv,
    r_send,
    r_recv,
    hidden_ref,
    gain_ref,
    router_ref,
    ids_ref,
    i_sem,
    extra,
    free_sem,
):
    tok, dim = hidden_hbm.shape
    half = tok // 2
    top_k = ids_hbm.shape[0]
    n_exp = wg_hbm.shape[0]
    inter = wg_hbm.shape[2]
    s_inter = sg_hbm.shape[1]
    chips = ep_size // 2
    far = chips // 2
    own_pos = 0
    far_pos = chips - 1
    n_groups = chips // 2
    group_rows = 4 * tok
    tiles_per_group = group_rows // LANES
    n_chunks = dim // COLS
    slots = n_exp * cap
    sh_steps = s_inter // LANES
    ex_steps = inter // LANES
    depth = dim // 2
    sh_halves = 2 * sh_steps
    ex_halves = n_exp * ex_steps
    w_steps = sh_halves + 2 * ex_halves
    d_per = n_exp + 2

    me = lax.axis_index("ep")
    core = lax.rem(me, 2)
    chip = me // 2
    partner = chip * 2 + (1 - core)

    def at_chip(delta, which):
        return lax.rem(chip + delta + chips, chips) * 2 + which

    def pos_of(way, hops):
        return far_pos if hops == far else 2 * hops - 1 + way

    def pos_at(delta):
        if delta == 0:
            return own_pos
        if abs(delta) == far:
            return far_pos
        return pos_of(0, delta) if delta > 0 else pos_of(1, -delta)

    def row_at(pos, which):
        return pos * 2 * tok + which * tok

    def w_pair(step):
        slot = lax.rem(step, STREAM_SLOTS)
        return slot

    def w_copies(slot, gate, up):
        return (
            pltpu.make_async_copy(gate, wbuf.at[slot, :, pl.ds(0, LANES)], w_sem.at[slot]),
            pltpu.make_async_copy(up, wbuf.at[slot, :, pl.ds(LANES, LANES)], w_sem.at[slot]),
        )

    def w_copies_shared(step):
        unit = step // 2
        rows = pl.ds(pl.multiple_of((step - 2 * unit) * depth, depth), depth)
        col = pl.ds(pl.multiple_of(unit * LANES, LANES), LANES)
        return w_copies(w_pair(step), sg_hbm.at[rows, col], su_hbm.at[rows, col])

    def w_copies_expert(step):
        rel = step - sh_halves
        part_k = rel // ex_halves
        rel = rel - part_k * ex_halves
        exp = rel // ex_steps
        rows = pl.ds(pl.multiple_of(part_k * depth, depth), depth)
        col = pl.ds(pl.multiple_of((rel - exp * ex_steps) * LANES, LANES), LANES)
        return w_copies(w_pair(step), wg_hbm.at[exp, rows, col], wu_hbm.at[exp, rows, col])

    def wait_bytes(ref, sem):
        pltpu.make_async_copy(ref, ref, sem).wait()

    def w_wait(step):
        slot = w_pair(step)
        wait_bytes(wbuf.at[slot], w_sem.at[slot])

    def w_start(step):
        @pl.when(step < sh_halves)
        def _():
            for copy in w_copies_shared(step):
                copy.start()

        @pl.when((step >= sh_halves) & (step < w_steps))
        def _():
            for copy in w_copies_expert(step):
                copy.start()

    def d_copy(chunk, which):
        slot = lax.rem(chunk, 2) * d_per + which
        col = pl.ds(pl.multiple_of(chunk * COLS, COLS), COLS)
        if which < n_exp:
            src = wd_hbm.at[which, :, col]
        else:
            src = sd_hbm.at[pl.ds((which - n_exp) * inter, inter), col]
        return pltpu.make_async_copy(src, dbuf.at[slot], d_sem.at[slot])

    def ag_copy(way, hops, k, u):
        src_row = row_at(own_pos if hops == 1 else pos_of(way, hops - 1), core) + u * half
        dst_row = row_at(pos_of(way, hops), core) + u * half
        cols = pl.ds(k * depth, depth)
        return pltpu.make_async_remote_copy(
            src_ref=xbuf.at[pl.ds(src_row, half), cols],
            dst_ref=xbuf.at[pl.ds(dst_row, half), cols],
            send_sem=ag_send,
            recv_sem=ag_recv.at[hops - 1, k, halves(way, hops).index(u)],
            device_id={"ep": at_chip(1 if way == 0 else -1, core)},
            device_id_type=MESH,
        )

    def cc_copy(way, hops, k, u, which):
        pos = own_pos if hops == 0 else pos_of(way, hops)
        rows = pl.ds(row_at(pos, which) + u * half, half)
        cols = pl.ds(k * depth, depth)
        return pltpu.make_async_remote_copy(
            src_ref=xbuf.at[rows, cols],
            dst_ref=xbuf.at[rows, cols],
            send_sem=cc_send,
            recv_sem=cc_recv.at[hops, k],
            device_id={"ep": partner},
            device_id_type=MESH,
        )

    def halves(way, hops):
        if hops == far:
            return (way,)
        return (0, 1) if way == 0 else (1, 0)

    def send_own(k, nth):
        for way in (0, 1):
            ag_copy(way, 1, k, halves(way, 1)[nth]).start()

    def relay(hops, k, nth):
        with jax.named_scope("relay"):
            wait_bytes(xbuf.at[pl.ds(0, tok), pl.ds(0, depth)], ag_recv.at[hops - 1, k, nth])
            for way in (0, 1):
                u = halves(way, hops)[nth]
                if hops < far and u in halves(way, hops + 1):
                    ag_copy(way, hops + 1, k, u).start()
                cc_copy(way, hops, k, u, core).start()

    def gate_copy(delta, other):
        dst_pos = pos_at(delta)
        dest = partner if delta == 0 else at_chip(delta, core if other == 0 else 1 - core)
        return pltpu.make_async_remote_copy(
            src_ref=gsend.at[dest],
            dst_ref=gmsg.at[dst_pos, core],
            send_sem=g_send,
            recv_sem=g_recv,
            device_id={"ep": dest},
            device_id_type=MESH,
        )

    deltas = [d for d in range(-(far - 1), far + 1)]

    barrier = pltpu.get_barrier_semaphore()
    for off in range(1, ep_size):
        pl.semaphore_signal(barrier, inc=1, device_id={"ep": lax.rem(me + off, ep_size)}, device_id_type=MESH)
    small = [
        pltpu.make_async_copy(src, dst, i_sem.at[k])
        for k, (src, dst) in enumerate(
            ((hidden_hbm, hidden_ref), (gain_hbm, gain_ref), (ids_hbm, ids_ref), (router_hbm, router_ref))
        )
    ]
    for copy in small:
        copy.start()
    small[0].wait()
    small[1].wait()

    x_f32 = hidden_ref[...].astype(F32)
    inv_rms = lax.rsqrt(jnp.mean(x_f32 * x_f32, axis=-1, keepdims=True) + NORM_EPS)
    x_norm = (x_f32 * inv_rms * gain_ref[...]).astype(BF16)
    own_row = row_at(own_pos, core)
    xbuf[pl.ds(pl.multiple_of(own_row, tok), tok), :] = x_norm

    with jax.named_scope("barrier"):
        pl.semaphore_wait(barrier, ep_size - 1)
    for nth in (0, 1):
        send_own(0, nth)
    for k in (0, 1):
        for u in (0, 1):
            cc_copy(0, 0, k, u, core).start()
    for step in range(STREAM_SLOTS):
        w_start(jnp.int32(step))

    with jax.named_scope("gates"):
        small[2].wait()
        small[3].wait()
        logits = lax.dot_general(
            router_ref[...],
            x_norm.astype(F32),
            (((1,), (1,)), ((), ())),
            precision=lax.Precision.HIGHEST,
            preferred_element_type=F32,
        )
        scores = jax.nn.sigmoid(logits)
        exp_iota = lax.broadcasted_iota(jnp.int32, scores.shape, 0)
        chosen = exp_iota == ids_ref[0:1, :]
        for k in range(1, top_k):
            chosen = chosen | (exp_iota == ids_ref[k : k + 1, :])
        total = jnp.sum(jnp.where(chosen, scores, 0.0), axis=0, keepdims=True)
        gates = jnp.where(chosen, ROUTE_SCALE * scores / total, -1.0)
        gates_t = jnp.concatenate([gates, jnp.full((gates.shape[0], LANES - tok), -1.0, F32)], axis=1)
        for dest in range(ep_size):
            piece = gates_t[dest * n_exp : (dest + 1) * n_exp, :]
            gsend[dest] = jnp.concatenate([piece, jnp.full((8 - n_exp, LANES), -1.0, F32)], axis=0)
        gmsg[own_pos, core] = gsend[me]
        for delta in deltas:
            for other in (0, 1):
                if delta == 0 and other == 0:
                    continue
                gate_copy(delta, other).start()

    for chunk in (0, 1):
        for which in range(d_per):
            d_copy(jnp.int32(chunk), which).start()

    def shared_step(unit, carry):
        steps = (2 * unit, 2 * unit + 1)
        for step in steps:
            w_wait(step)
        rows = pl.ds(pl.multiple_of(own_row, tok), tok)
        both = jnp.dot(xbuf[rows, :depth], wbuf[w_pair(steps[0])], preferred_element_type=F32)
        both = both + jnp.dot(xbuf[rows, depth:], wbuf[w_pair(steps[1])], preferred_element_type=F32)
        act = (jax.nn.silu(both[:, :LANES]) * both[:, LANES:]).astype(BF16)
        shid[:, pl.ds(pl.multiple_of(unit * LANES, LANES), LANES)] = act
        for step in steps:
            w_start(step + STREAM_SLOTS)
        return carry

    def shared_steps(lo, hi):
        with jax.named_scope("shared"):
            lax.fori_loop(min(lo, sh_steps), min(hi, sh_steps), shared_step, 0)

    shared_steps(0, 7)
    relay(1, 0, 0)
    shared_steps(7, 11)
    relay(1, 0, 1)
    send_own(1, 0)

    wait_bytes(gsend.at[pl.ds(0, ep_size - 1)], g_recv)

    lane = lax.broadcasted_iota(jnp.int32, (8, LANES), 1)
    packed = []
    for g in range(n_groups):
        b0, b1, b2, b3 = gmsg[2 * g, 0], gmsg[2 * g, 1], gmsg[2 * g + 1, 0], gmsg[2 * g + 1, 1]
        r1 = pltpu.roll(b1, 96, 1)
        r2 = pltpu.roll(b2, 64, 1)
        r3 = pltpu.roll(b3, 32, 1)
        packed.append(jnp.where(lane < 96, b0, r1))
        packed.append(jnp.where(lane < 64, r1, r2))
        packed.append(jnp.where(lane < 32, r2, r3))
    n_tiles = len(packed)
    member = jnp.concatenate([jnp.where(p < 0, 0.0, 1.0) for p in packed], axis=0)
    upper = jnp.where(
        lax.broadcasted_iota(jnp.int32, (LANES, LANES), 0) < lax.broadcasted_iota(jnp.int32, (LANES, LANES), 1), 1.0, 0.0
    ).astype(BF16)
    within = jnp.dot(member.astype(BF16), upper, preferred_element_type=F32)
    base = jnp.zeros((8, 1), F32)
    for t in range(n_tiles):
        m = member[t * 8 : (t + 1) * 8]
        rank = jnp.where(m > 0, within[t * 8 : (t + 1) * 8] + base, -1.0)
        base = base + jnp.sum(m, axis=1, keepdims=True)
        rank_ref[t] = rank
        both = jnp.concatenate([rank, packed[t], jnp.zeros((LANES - 16, LANES), F32)], axis=0)
        cols_ref[t * LANES : (t + 1) * LANES, :] = jnp.transpose(both)

    slot_rows = lax.broadcasted_iota(jnp.int32, (cap, LANES), 0).astype(F32)
    slot_lanes = lax.broadcasted_iota(jnp.int32, (LANES, cap), 1).astype(F32)

    def build(t, carry):
        rank = rank_ref[t]
        col = cols_ref[pl.ds(pl.multiple_of(t * LANES, LANES), LANES), :]
        for e in range(n_exp):
            hot = jnp.where(slot_rows == rank[e : e + 1, :], 1.0, 0.0)
            pick[e * cap : (e + 1) * cap, pl.ds(pl.multiple_of(t * LANES, LANES), LANES)] = hot.astype(BF16)
            hot_t = jnp.where(slot_lanes == col[:, e : e + 1], 1.0, 0.0)
            place[pl.ds(pl.multiple_of(t * LANES, LANES), LANES), e * cap : (e + 1) * cap] = hot_t.astype(BF16)
        return carry

    relay(2, 0, 0)
    with jax.named_scope("build"):
        lax.fori_loop(0, n_tiles, build, 0)
    relay(2, 0, 1)
    send_own(1, 1)

    def gather_rows(k, first, last):
        lo = 0 if first == 0 else rows_within(first)
        hi = rows_within(last)

        def body(n, carry):
            cols = pl.ds(pl.multiple_of(n * 2 * COLS, 2 * COLS), 2 * COLS)
            rows = xbuf[lo:hi, cols]
            for e in range(n_exp):
                got = jnp.dot(pick[e * cap : (e + 1) * cap, lo:hi], rows, preferred_element_type=F32).astype(BF16)
                if lo > 0:
                    got = got + xg[e * cap : (e + 1) * cap, cols]
                xg[e * cap : (e + 1) * cap, cols] = got
            return carry

        with jax.named_scope("gather"):
            lax.fori_loop(k * n_chunks // 4, (k + 1) * n_chunks // 4, body, 0)

    def wait_from_core(hops, k):
        with jax.named_scope("from_core"):
            n_rows = 2 * tok if 0 < hops < far else tok
            wait_bytes(xbuf.at[pl.ds(0, n_rows), pl.ds(0, depth)], cc_recv.at[hops, k])

    def rows_within(hops):
        return (2 * tok * (1 + 2 * hops)) // COLS * COLS if hops < far else chips * 2 * tok

    def kept(j, exp):
        if j < 4:
            return from_core.at[2 * exp + j // 2, pl.ds(4 * (j % 2), 4)]
        if j < 8:
            return ring.at[2 * exp + (j - 4) // 2, j % 2]
        if j < 10:
            return part.at[j - 8, pl.ds(2 * exp, 2)]
        return extra.at[exp]

    def up_half(k, between):
        def up_expert(exp, carry):
            rows = pl.ds(pl.multiple_of(exp * cap, cap), cap)
            first = sh_halves + k * ex_halves + exp * ex_steps
            for lo in range(0, ex_steps, STEP_UNITS):
                units = range(lo, min(lo + STEP_UNITS, ex_steps))
                with jax.named_scope("up"):
                    for j in units:
                        w_wait(first + j)
                    for j in units:
                        both = jnp.dot(
                            xg[rows, k * depth : (k + 1) * depth], wbuf[w_pair(first + j)], preferred_element_type=F32
                        )
                        view = kept(j, exp)
                        if k == 0:
                            view[...] = both.reshape(view.shape)
                        else:
                            both = both + view[...].reshape(both.shape)
                            act = (jax.nn.silu(both[:, :LANES]) * both[:, LANES:]).astype(BF16)
                            hid[rows, j * LANES : (j + 1) * LANES] = act
                    for j in units:
                        w_start(first + j + STREAM_SLOTS)
                for at, events in between.items():
                    if at[1] == min(lo // STEP_UNITS, 1):
                        @pl.when(exp == at[0])
                        def _():
                            for event in events:
                                relay(*event)
            return carry

        lax.fori_loop(0, n_exp, up_expert, 0)

    wait_from_core(0, 0)
    wait_from_core(1, 0)
    gather_rows(0, 0, 1)
    wait_from_core(2, 0)
    gather_rows(0, 1, 2)
    shared_steps(11, 13)
    relay(3, 0, 0)
    relay(1, 1, 0)
    shared_steps(13, 18)
    relay(3, 0, 1)
    shared_steps(18, 20)
    wait_from_core(3, 0)
    gather_rows(0, 2, 3)
    relay(1, 1, 1)
    shared_steps(20, sh_steps)
    relay(4, 0, 0)
    wait_from_core(0, 1)
    wait_from_core(1, 1)
    gather_rows(1, 0, 1)
    wait_from_core(4, 0)
    relay(2, 1, 0)
    gather_rows(0, 3, 4)
    up_half(
        0,
        {
            (0, 0): [(2, 1, 1)],
            (1, 0): [(3, 1, 0)],
            (2, 0): [(3, 1, 1)],
            (3, 0): [(4, 1, 0)],
        },
    )
    for hops in range(2, far + 1):
        wait_from_core(hops, 1)
    gather_rows(1, 1, 4)
    up_half(1, {})

    pl.semaphore_signal(free_sem.at[0], inc=1, device_id={"ep": partner}, device_id_type=MESH)
    pl.semaphore_signal(free_sem.at[1], inc=1, device_id={"ep": at_chip(-1, core)}, device_id_type=MESH)
    pl.semaphore_signal(free_sem.at[2], inc=1, device_id={"ep": at_chip(1, core)}, device_id_type=MESH)

    def part_copy(chunk, rest):
        par = lax.rem(chunk, 2)
        which = pl.ds(0, far_pos) if rest else pl.ds(far_pos, 1)
        return pltpu.make_async_remote_copy(
            src_ref=part.at[par, which, 1 - core],
            dst_ref=from_core.at[chunk, which],
            send_sem=p_send.at[par],
            recv_sem=p_recv.at[chunk, rest],
            device_id={"ep": partner},
            device_id_type=MESH,
        )

    def part_sent(chunk):
        par = lax.rem(chunk, 2)
        wait_bytes(part.at[par, :, 0], p_send.at[par])

    def ring_copy(chunk, way, hop):
        dev = {"ep": at_chip(1 if way == 0 else -1, core)}
        if hop == 1:
            src = from_core.at[chunk, far_pos, pl.ds(way * half, half), :]
            dst = ring.at[chunk, way, 0, pl.ds(way * half, half), :]
        else:
            src = ring.at[chunk, way, hop - 2]
            dst = ring.at[chunk, way, hop - 1]
        return pltpu.make_async_remote_copy(
            src_ref=src,
            dst_ref=dst,
            send_sem=r_send.at[chunk],
            recv_sem=r_recv.at[chunk, hop - 1],
            device_id=dev,
            device_id_type=MESH,
        )

    def dest_pos(way, hops):
        return pos_of(1 - way, hops)

    def down(chunk):
        par = lax.rem(chunk, 2)
        for which in range(d_per):
            d_copy(chunk, which).wait()
        for e in range(n_exp):
            got = jnp.dot(hid[e * cap : (e + 1) * cap, :], dbuf[par * d_per + e], preferred_element_type=F32)
            erows[e * cap : (e + 1) * cap, :] = got.astype(BF16)
        shared = jnp.dot(shid[:, :inter], dbuf[par * d_per + n_exp], preferred_element_type=F32)
        shared = shared + jnp.dot(shid[:, inter:], dbuf[par * d_per + n_exp + 1], preferred_element_type=F32)
        sout[:, pl.ds(pl.multiple_of(chunk * COLS, COLS), COLS)] = shared.astype(BF16)

        @pl.when(chunk + 2 < n_chunks)
        def _():
            for which in range(d_per):
                d_copy(chunk + 2, which).start()

    def combine(chunk, groups):
        par = lax.rem(chunk, 2)
        for g in groups:
            rows = slice(g * group_rows, (g + 1) * group_rows)
            acc = None
            for e in range(n_exp):
                got = jnp.dot(
                    place[rows, e * cap : (e + 1) * cap], erows[e * cap : (e + 1) * cap, :], preferred_element_type=F32
                )
                got = cols_ref[rows, 8 + e : 9 + e] * got
                acc = got if acc is None else acc + got
            for b in range(4):
                part[par, 2 * g + b // 2, b % 2] = acc[b * tok : (b + 1) * tok]

    def fold_rest(chunk):
        par = lax.rem(chunk, 2)
        part_copy(chunk, 1).wait_recv()
        for pos in range(far_pos):
            from_core[chunk, pos] = from_core[chunk, pos] + part[par, pos, core]

    def first_hop(chunk):
        par = lax.rem(chunk, 2)
        part_copy(chunk, 0).wait_recv()
        from_core[chunk, far_pos] = from_core[chunk, far_pos] + part[par, far_pos, core]

        @pl.when(chunk == 0)
        def _():
            pl.semaphore_wait(free_sem.at[1], 1)
            pl.semaphore_wait(free_sem.at[2], 1)

        for way in (0, 1):
            ring_copy(chunk, way, 1).start()

    def ring_arrived(chunk, hop):
        wait_bytes(ring.at[chunk, 0, 0] if hop == 1 else ring.at[chunk, :, 0], r_recv.at[chunk, hop - 1])

    def pass_on(chunk, hop):
        ring_arrived(chunk, hop)
        for way in (0, 1):
            pos = dest_pos(way, far - hop)
            if hop == 1:
                done = pl.ds(way * half, half)
                rest = pl.ds((1 - way) * half, half)
                ring[chunk, way, 0, done, :] = ring[chunk, way, 0, done, :] + from_core[chunk, pos, done, :]
                ring[chunk, way, 0, rest, :] = from_core[chunk, pos, rest, :]
            else:
                ring[chunk, way, hop - 1] = ring[chunk, way, hop - 1] + from_core[chunk, pos]
            ring_copy(chunk, way, hop + 1).start()

    def finish(chunk):
        cols = pl.ds(pl.multiple_of(chunk * COLS, COLS), COLS)
        ring_arrived(chunk, far)
        routed = from_core[chunk, own_pos] + ring[chunk, 0, far - 1] + ring[chunk, 1, far - 1]
        out_ref[:, cols] = (hidden_ref[:, cols].astype(F32) + sout[:, cols].astype(F32) + routed).astype(BF16)

        @pl.when(chunk >= 1)
        def _():
            ring_sends_done(chunk - 1)

    def ring_sends_done(chunk):
        wait_bytes(from_core.at[chunk, pl.ds(0, 2 * far - 1)], r_send.at[chunk])

    def gather_sends_done():
        wait_bytes(xbuf.at[pl.ds(0, (chips - 1) * tok), :], ag_send)
        wait_bytes(xbuf.at[pl.ds(0, chips * tok), :], cc_send)
        wait_bytes(gsend.at[pl.ds(0, ep_size - 1)], g_send)

    def turn(i, carry):
        def for_chunk(lag, name, fn):
            @pl.when((i >= lag) & (i - lag < n_chunks))
            def _():
                with jax.named_scope(name):
                    fn(i - lag)

        def hops_of(in_middle):
            for hop in range(1, far + 1):
                if (hop % 2 == 0) == in_middle:
                    lag = 3 * hop // 2 if in_middle else (3 * hop - 1) // 2
                    if hop == far:
                        for_chunk(lag, "finish", finish)
                    else:
                        for_chunk(lag, "pass_on", functools.partial(pass_on, hop=hop))

        for_chunk(0, "down", down)
        for_chunk(1, "fold_rest", fold_rest)
        hops_of(True)

        @pl.when(i < n_chunks)
        def _():
            @pl.when(i >= 2)
            def _():
                part_sent(i)

            with jax.named_scope("combine_far"):
                combine(i, (n_groups - 1,))

                @pl.when(i == 0)
                def _():
                    pl.semaphore_wait(free_sem.at[0], 1)

                part_copy(i, 0).start()
            with jax.named_scope("combine"):
                combine(i, range(n_groups - 1))
                part_copy(i, 1).start()

        for_chunk(0, "first_hop", first_hop)
        hops_of(False)

        @pl.when(i == n_chunks)
        def _():
            gather_sends_done()

        return carry

    lax.fori_loop(0, n_chunks + 3 * far // 2, turn, 0)

    for par in (0, 1):
        part_sent(par)
    ring_sends_done(jnp.int32(n_chunks - 1))


def solution(mesh):
    ep_size = mesh.shape["ep"]

    def local_block(hidden_in, norm_gain, router_w, w_gate, w_up, w_down, ws_gate, ws_up, ws_down, expert_ids):
        tok, top_k = expert_ids.shape
        dim = hidden_in.shape[1]
        n_exp, _, inter = w_gate.shape
        s_inter = ws_gate.shape[1]
        chips = ep_size // 2
        far = chips // 2
        n_chunks = dim // COLS
        pair_cap = GROUPS * ((top_k + GROUP_LIMIT - 1) // GROUP_LIMIT) * tok // ep_size
        cap = pair_cap * ep_size // n_exp
        all_tok = ep_size * tok
        slots = n_exp * cap
        n_tiles = all_tok // LANES
        vmem = pl.BlockSpec(memory_space=pltpu.VMEM)
        hbm = pl.BlockSpec(memory_space=pl.ANY)
        dma = pltpu.SemaphoreType.DMA
        return pl.pallas_call(
            functools.partial(moe_kernel, ep_size, cap),
            out_shape=pltpu.VMEM((tok, dim), BF16),
            in_specs=[hbm] * 10,
            out_specs=vmem,
            scratch_shapes=[
                pltpu.VMEM((all_tok, dim), BF16),
                pltpu.VMEM((ep_size, 8, LANES), F32),
                pltpu.VMEM((chips, 2, 8, LANES), F32),
                pltpu.VMEM((n_tiles, 8, LANES), F32),
                pltpu.VMEM((all_tok, LANES), F32),
                pltpu.VMEM((slots, all_tok), BF16),
                pltpu.VMEM((all_tok, slots), BF16),
                pltpu.VMEM((slots, dim), BF16),
                pltpu.VMEM((slots, inter), BF16),
                pltpu.VMEM((tok, s_inter), BF16),
                pltpu.VMEM((tok, dim), BF16),
                pltpu.VMEM((STREAM_SLOTS, dim // 2, 2 * LANES), BF16),
                pltpu.VMEM((2 * (n_exp + 2), inter, COLS), BF16),
                pltpu.VMEM((2, chips, 2, tok, COLS), F32),
                pltpu.VMEM((slots, COLS), BF16),
                pltpu.VMEM((n_chunks, chips, tok, COLS), F32),
                pltpu.VMEM((n_chunks, 2, far, tok, COLS), F32),
                dma((STREAM_SLOTS,)),
                dma((2 * (n_exp + 2),)),
                dma,
                dma((far, 2, 2)),
                dma,
                dma((far + 1, 2)),
                dma,
                dma,
                dma((2,)),
                dma((n_chunks, 2)),
                dma((n_chunks,)),
                dma((n_chunks, far)),
                pltpu.VMEM((tok, dim), BF16),
                pltpu.VMEM((1, dim), F32),
                pltpu.VMEM(router_w.shape, F32),
                pltpu.VMEM((top_k, tok), jnp.int32),
                dma((4,)),
                pltpu.VMEM((n_exp, cap, COLS), F32),
                pltpu.SemaphoreType.REGULAR((3,)),
            ],
            compiler_params=pltpu.CompilerParams(
                collective_id=0, has_side_effects=True, vmem_limit_bytes=66500000
            ),
        )(hidden_in, norm_gain.reshape(1, dim), router_w, expert_ids.T, w_gate, w_up, w_down, ws_gate, ws_up, ws_down)

    row_spec = P(("dp", "ep"), None)
    in_specs = (row_spec, P(), P(), P("ep"), P("ep"), P("ep"), P(), P(), P(), row_spec)
    return jax.shard_map(local_block, mesh=mesh, in_specs=in_specs, out_specs=row_spec, check_vma=False)
```

```python
import functools

import jax
import jax.numpy as jnp
from jax import lax
from jax.experimental import pallas as pl
from jax.experimental.pallas import tpu as pltpu
from jax.sharding import PartitionSpec as P

NORM_EPS = 1e-6
ROUTE_SCALE = 2.5
GROUPS = 8
GROUP_LIMIT = 4
LANES = 128
COLS = 256
STREAM_SLOTS = 16
MESH = pl.DeviceIdType.MESH
F32 = jnp.float32
BF16 = jnp.bfloat16


def moe_kernel(
    ep_size,
    cap,
    hidden_hbm,
    gain_hbm,
    router_hbm,
    ids_hbm,
    wg_hbm,
    wu_hbm,
    wd_hbm,
    sg_hbm,
    su_hbm,
    sd_hbm,
    out_ref,
    xbuf,
    gsend,
    gmsg,
    rank_ref,
    cols_ref,
    pick,
    place,
    xg,
    hid,
    shid,
    sout,
    wbuf,
    dbuf,
    part,
    erows,
    from_core,
    ring,
    w_sem,
    d_sem,
    ag_send,
    ag_recv,
    cc_send,
    cc_recv,
    g_send,
    g_recv,
    p_send,
    p_recv,
    r_send,
    r_recv,
    hidden_ref,
    gain_ref,
    router_ref,
    ids_ref,
    i_sem,
    extra,
    free_sem,
):
    tok, dim = hidden_hbm.shape
    half = tok // 2
    top_k = ids_hbm.shape[0]
    n_exp = wg_hbm.shape[0]
    inter = wg_hbm.shape[2]
    s_inter = sg_hbm.shape[1]
    chips = ep_size // 2
    far = chips // 2
    own_pos = 0
    far_pos = chips - 1
    n_groups = chips // 2
    group_rows = 4 * tok
    tiles_per_group = group_rows // LANES
    n_chunks = dim // COLS
    slots = n_exp * cap
    sh_steps = s_inter // LANES
    ex_steps = inter // LANES
    depth = dim // 2
    sh_halves = 2 * sh_steps
    ex_halves = n_exp * ex_steps
    w_steps = sh_halves + 2 * ex_halves
    d_per = n_exp + 2

    me = lax.axis_index("ep")
    core = lax.rem(me, 2)
    chip = me // 2
    partner = chip * 2 + (1 - core)

    def at_chip(delta, which):
        return lax.rem(chip + delta + chips, chips) * 2 + which

    def pos_of(way, hops):
        return far_pos if hops == far else 2 * hops - 1 + way

    def pos_at(delta):
        if delta == 0:
            return own_pos
        if abs(delta) == far:
            return far_pos
        return pos_of(0, delta) if delta > 0 else pos_of(1, -delta)

    def row_at(pos, which):
        return pos * 2 * tok + which * tok

    def w_pair(step):
        slot = lax.rem(step, STREAM_SLOTS)
        return slot

    def w_copies(slot, gate, up):
        return (
            pltpu.make_async_copy(gate, wbuf.at[slot, :, pl.ds(0, LANES)], w_sem.at[slot]),
            pltpu.make_async_copy(up, wbuf.at[slot, :, pl.ds(LANES, LANES)], w_sem.at[slot]),
        )

    def w_copies_shared(step):
        unit = step // 2
        rows = pl.ds(pl.multiple_of((step - 2 * unit) * depth, depth), depth)
        col = pl.ds(pl.multiple_of(unit * LANES, LANES), LANES)
        return w_copies(w_pair(step), sg_hbm.at[rows, col], su_hbm.at[rows, col])

    def w_copies_expert(step):
        rel = step - sh_halves
        part_k = rel // ex_halves
        rel = rel - part_k * ex_halves
        exp = rel // ex_steps
        rows = pl.ds(pl.multiple_of(part_k * depth, depth), depth)
        col = pl.ds(pl.multiple_of((rel - exp * ex_steps) * LANES, LANES), LANES)
        return w_copies(w_pair(step), wg_hbm.at[exp, rows, col], wu_hbm.at[exp, rows, col])

    def wait_bytes(ref, sem):
        pltpu.make_async_copy(ref, ref, sem).wait()

    def w_wait(step):
        slot = w_pair(step)
        wait_bytes(wbuf.at[slot], w_sem.at[slot])

    def w_start(step):
        @pl.when(step < sh_halves)
        def _():
            for copy in w_copies_shared(step):
                copy.start()

        @pl.when((step >= sh_halves) & (step < w_steps))
        def _():
            for copy in w_copies_expert(step):
                copy.start()

    def d_copy(chunk, which):
        slot = lax.rem(chunk, 2) * d_per + which
        col = pl.ds(pl.multiple_of(chunk * COLS, COLS), COLS)
        if which < n_exp:
            src = wd_hbm.at[which, :, col]
        else:
            src = sd_hbm.at[pl.ds((which - n_exp) * inter, inter), col]
        return pltpu.make_async_copy(src, dbuf.at[slot], d_sem.at[slot])

    def ag_copy(way, hops, k, u):
        src_row = row_at(own_pos if hops == 1 else pos_of(way, hops - 1), core) + u * half
        dst_row = row_at(pos_of(way, hops), core) + u * half
        cols = pl.ds(k * depth, depth)
        return pltpu.make_async_remote_copy(
            src_ref=xbuf.at[pl.ds(src_row, half), cols],
            dst_ref=xbuf.at[pl.ds(dst_row, half), cols],
            send_sem=ag_send,
            recv_sem=ag_recv.at[hops - 1, k, halves(way, hops).index(u)],
            device_id={"ep": at_chip(1 if way == 0 else -1, core)},
            device_id_type=MESH,
        )

    def cc_copy(way, hops, k, u, which):
        pos = own_pos if hops == 0 else pos_of(way, hops)
        rows = pl.ds(row_at(pos, which) + u * half, half)
        cols = pl.ds(k * depth, depth)
        return pltpu.make_async_remote_copy(
            src_ref=xbuf.at[rows, cols],
            dst_ref=xbuf.at[rows, cols],
            send_sem=cc_send,
            recv_sem=cc_recv.at[hops, k],
            device_id={"ep": partner},
            device_id_type=MESH,
        )

    def halves(way, hops):
        if hops == far:
            return (way,)
        return (0, 1) if way == 0 else (1, 0)

    def send_own(k, nth):
        for way in (0, 1):
            ag_copy(way, 1, k, halves(way, 1)[nth]).start()

    def relay(hops, k, nth):
        with jax.named_scope("relay"):
            wait_bytes(xbuf.at[pl.ds(0, tok), pl.ds(0, depth)], ag_recv.at[hops - 1, k, nth])
            for way in (0, 1):
                u = halves(way, hops)[nth]
                if hops < far and u in halves(way, hops + 1):
                    ag_copy(way, hops + 1, k, u).start()
                cc_copy(way, hops, k, u, core).start()

    def gate_copy(delta, other):
        dst_pos = pos_at(delta)
        dest = partner if delta == 0 else at_chip(delta, core if other == 0 else 1 - core)
        return pltpu.make_async_remote_copy(
            src_ref=gsend.at[dest],
            dst_ref=gmsg.at[dst_pos, core],
            send_sem=g_send,
            recv_sem=g_recv,
            device_id={"ep": dest},
            device_id_type=MESH,
        )

    deltas = [d for d in range(-(far - 1), far + 1)]

    barrier = pltpu.get_barrier_semaphore()
    for off in range(1, ep_size):
        pl.semaphore_signal(barrier, inc=1, device_id={"ep": lax.rem(me + off, ep_size)}, device_id_type=MESH)
    small = [
        pltpu.make_async_copy(src, dst, i_sem.at[k])
        for k, (src, dst) in enumerate(
            ((hidden_hbm, hidden_ref), (gain_hbm, gain_ref), (ids_hbm, ids_ref), (router_hbm, router_ref))
        )
    ]
    for copy in small:
        copy.start()
    small[0].wait()
    small[1].wait()

    x_f32 = hidden_ref[...].astype(F32)
    inv_rms = lax.rsqrt(jnp.mean(x_f32 * x_f32, axis=-1, keepdims=True) + NORM_EPS)
    x_norm = (x_f32 * inv_rms * gain_ref[...]).astype(BF16)
    own_row = row_at(own_pos, core)
    xbuf[pl.ds(pl.multiple_of(own_row, tok), tok), :] = x_norm

    with jax.named_scope("barrier"):
        pl.semaphore_wait(barrier, ep_size - 1)
    for nth in (0, 1):
        send_own(0, nth)
    for k in (0, 1):
        for u in (0, 1):
            cc_copy(0, 0, k, u, core).start()
    for step in range(STREAM_SLOTS):
        w_start(jnp.int32(step))

    with jax.named_scope("gates"):
        small[2].wait()
        small[3].wait()
        logits = lax.dot_general(
            router_ref[...],
            x_norm.astype(F32),
            (((1,), (1,)), ((), ())),
            precision=lax.Precision.HIGHEST,
            preferred_element_type=F32,
        )
        scores = jax.nn.sigmoid(logits)
        exp_iota = lax.broadcasted_iota(jnp.int32, scores.shape, 0)
        chosen = exp_iota == ids_ref[0:1, :]
        for k in range(1, top_k):
            chosen = chosen | (exp_iota == ids_ref[k : k + 1, :])
        total = jnp.sum(jnp.where(chosen, scores, 0.0), axis=0, keepdims=True)
        gates = jnp.where(chosen, ROUTE_SCALE * scores / total, -1.0)
        gates_t = jnp.concatenate([gates, jnp.full((gates.shape[0], LANES - tok), -1.0, F32)], axis=1)
        for dest in range(ep_size):
            piece = gates_t[dest * n_exp : (dest + 1) * n_exp, :]
            gsend[dest] = jnp.concatenate([piece, jnp.full((8 - n_exp, LANES), -1.0, F32)], axis=0)
        gmsg[own_pos, core] = gsend[me]
        for delta in deltas:
            for other in (0, 1):
                if delta == 0 and other == 0:
                    continue
                gate_copy(delta, other).start()

    for chunk in (0, 1):
        for which in range(d_per):
            d_copy(jnp.int32(chunk), which).start()

    def shared_step(unit, carry):
        steps = (2 * unit, 2 * unit + 1)
        for step in steps:
            w_wait(step)
        rows = pl.ds(pl.multiple_of(own_row, tok), tok)
        both = jnp.dot(xbuf[rows, :depth], wbuf[w_pair(steps[0])], preferred_element_type=F32)
        both = both + jnp.dot(xbuf[rows, depth:], wbuf[w_pair(steps[1])], preferred_element_type=F32)
        act = (jax.nn.silu(both[:, :LANES]) * both[:, LANES:]).astype(BF16)
        shid[:, pl.ds(pl.multiple_of(unit * LANES, LANES), LANES)] = act
        for step in steps:
            w_start(step + STREAM_SLOTS)
        return carry

    def shared_steps(lo, hi):
        with jax.named_scope("shared"):
            lax.fori_loop(min(lo, sh_steps), min(hi, sh_steps), shared_step, 0)

    shared_steps(0, 7)
    relay(1, 0, 0)
    shared_steps(7, 11)
    relay(1, 0, 1)
    send_own(1, 0)

    wait_bytes(gsend.at[pl.ds(0, ep_size - 1)], g_recv)

    lane = lax.broadcasted_iota(jnp.int32, (8, LANES), 1)
    packed = []
    for g in range(n_groups):
        b0, b1, b2, b3 = gmsg[2 * g, 0], gmsg[2 * g, 1], gmsg[2 * g + 1, 0], gmsg[2 * g + 1, 1]
        r1 = pltpu.roll(b1, 96, 1)
        r2 = pltpu.roll(b2, 64, 1)
        r3 = pltpu.roll(b3, 32, 1)
        packed.append(jnp.where(lane < 96, b0, r1))
        packed.append(jnp.where(lane < 64, r1, r2))
        packed.append(jnp.where(lane < 32, r2, r3))
    n_tiles = len(packed)
    member = jnp.concatenate([jnp.where(p < 0, 0.0, 1.0) for p in packed], axis=0)
    upper = jnp.where(
        lax.broadcasted_iota(jnp.int32, (LANES, LANES), 0) < lax.broadcasted_iota(jnp.int32, (LANES, LANES), 1), 1.0, 0.0
    ).astype(BF16)
    within = jnp.dot(member.astype(BF16), upper, preferred_element_type=F32)
    base = jnp.zeros((8, 1), F32)
    for t in range(n_tiles):
        m = member[t * 8 : (t + 1) * 8]
        rank = jnp.where(m > 0, within[t * 8 : (t + 1) * 8] + base, -1.0)
        base = base + jnp.sum(m, axis=1, keepdims=True)
        rank_ref[t] = rank
        both = jnp.concatenate([rank, packed[t], jnp.zeros((LANES - 16, LANES), F32)], axis=0)
        cols_ref[t * LANES : (t + 1) * LANES, :] = jnp.transpose(both)

    slot_rows = lax.broadcasted_iota(jnp.int32, (cap, LANES), 0).astype(F32)
    slot_lanes = lax.broadcasted_iota(jnp.int32, (LANES, cap), 1).astype(F32)

    def build(t, carry):
        rank = rank_ref[t]
        col = cols_ref[pl.ds(pl.multiple_of(t * LANES, LANES), LANES), :]
        for e in range(n_exp):
            hot = jnp.where(slot_rows == rank[e : e + 1, :], 1.0, 0.0)
            pick[e * cap : (e + 1) * cap, pl.ds(pl.multiple_of(t * LANES, LANES), LANES)] = hot.astype(BF16)
            hot_t = jnp.where(slot_lanes == col[:, e : e + 1], 1.0, 0.0)
            place[pl.ds(pl.multiple_of(t * LANES, LANES), LANES), e * cap : (e + 1) * cap] = hot_t.astype(BF16)
        return carry

    relay(2, 0, 0)
    with jax.named_scope("build"):
        lax.fori_loop(0, n_tiles, build, 0)
    relay(2, 0, 1)
    send_own(1, 1)

    def gather_rows(k, first, last):
        lo = 0 if first == 0 else rows_within(first)
        hi = rows_within(last)

        def body(n, carry):
            cols = pl.ds(pl.multiple_of(n * 2 * COLS, 2 * COLS), 2 * COLS)
            rows = xbuf[lo:hi, cols]
            for e in range(n_exp):
                got = jnp.dot(pick[e * cap : (e + 1) * cap, lo:hi], rows, preferred_element_type=F32).astype(BF16)
                if lo > 0:
                    got = got + xg[e * cap : (e + 1) * cap, cols]
                xg[e * cap : (e + 1) * cap, cols] = got
            return carry

        with jax.named_scope("gather"):
            lax.fori_loop(k * n_chunks // 4, (k + 1) * n_chunks // 4, body, 0)

    def wait_from_core(hops, k):
        with jax.named_scope("from_core"):
            n_rows = 2 * tok if 0 < hops < far else tok
            wait_bytes(xbuf.at[pl.ds(0, n_rows), pl.ds(0, depth)], cc_recv.at[hops, k])

    def rows_within(hops):
        return (2 * tok * (1 + 2 * hops)) // COLS * COLS if hops < far else chips * 2 * tok

    def kept(j, exp):
        if j < 4:
            return from_core.at[2 * exp + j // 2, pl.ds(4 * (j % 2), 4)]
        if j < 8:
            return ring.at[2 * exp + (j - 4) // 2, j % 2]
        if j < 10:
            return part.at[j - 8, pl.ds(2 * exp, 2)]
        return extra.at[exp]

    def up_first(exp, carry):
        rows = pl.ds(pl.multiple_of(exp * cap, cap), cap)
        first = sh_halves + exp * ex_steps
        with jax.named_scope("up_first"):
            for j in range(ex_steps):
                w_wait(first + j)
            for j in range(ex_steps):
                slot = w_pair(first + j)
                both = jnp.dot(xg[rows, :depth], wbuf[slot], preferred_element_type=F32)
                view = kept(j, exp)
                view[...] = both.reshape(view.shape)
                then = exp + (j + STREAM_SLOTS) // ex_steps
                wrap = then // n_exp
                then = then - wrap * n_exp
                deep = pl.ds(pl.multiple_of(wrap * depth, depth), depth)
                col = pl.ds((j + STREAM_SLOTS) % ex_steps * LANES, LANES)
                for copy in w_copies(slot, wg_hbm.at[then, deep, col], wu_hbm.at[then, deep, col]):
                    copy.start()
        for at, event in enumerate(((2, 1, 1), (3, 1, 0), (3, 1, 1), (4, 1, 0))):
            @pl.when(exp == at)
            def _():
                relay(*event)
        return carry

    wait_from_core(0, 0)
    wait_from_core(1, 0)
    gather_rows(0, 0, 1)
    wait_from_core(2, 0)
    gather_rows(0, 1, 2)
    shared_steps(11, 13)
    relay(3, 0, 0)
    relay(1, 1, 0)
    shared_steps(13, 18)
    relay(3, 0, 1)
    shared_steps(18, 20)
    wait_from_core(3, 0)
    gather_rows(0, 2, 3)
    relay(1, 1, 1)
    shared_steps(20, sh_steps)
    relay(4, 0, 0)
    wait_from_core(0, 1)
    wait_from_core(1, 1)
    gather_rows(1, 0, 1)
    wait_from_core(4, 0)
    relay(2, 1, 0)
    gather_rows(0, 3, 4)
    lax.fori_loop(0, n_exp, up_first, 0)
    wait_from_core(2, 1)
    wait_from_core(3, 1)
    gather_rows(1, 1, 3)
    wait_from_core(4, 1)
    gather_rows(1, 3, 4)
    def up_rest(exp, refill):
        rows = pl.ds(pl.multiple_of(exp * cap, cap), cap)
        first = sh_halves + ex_halves + exp * ex_steps
        with jax.named_scope("up_rest"):
            for j in range(ex_steps):
                w_wait(first + j)
            for j in range(ex_steps):
                slot = w_pair(first + j)
                both = jnp.dot(xg[rows, depth:], wbuf[slot], preferred_element_type=F32)
                view = kept(j, exp)
                both = both + view[...].reshape(both.shape)
                act = (jax.nn.silu(both[:, :LANES]) * both[:, LANES:]).astype(BF16)
                hid[rows, j * LANES : (j + 1) * LANES] = act
                low = pl.ds(depth, depth)
                ahead = (j + STREAM_SLOTS) // ex_steps
                if ahead <= refill:
                    col = pl.ds((j + STREAM_SLOTS) % ex_steps * LANES, LANES)
                    for copy in w_copies(slot, wg_hbm.at[exp + ahead, low, col], wu_hbm.at[exp + ahead, low, col]):
                        copy.start()

    furthest = (ex_steps - 1 + STREAM_SLOTS) // ex_steps

    def up_rest_step(exp, carry):
        up_rest(exp, furthest)
        return carry

    lax.fori_loop(0, n_exp - furthest, up_rest_step, 0)
    for exp in range(n_exp - furthest, n_exp):
        up_rest(jnp.int32(exp), n_exp - 1 - exp)

    pl.semaphore_signal(free_sem.at[0], inc=1, device_id={"ep": partner}, device_id_type=MESH)
    pl.semaphore_signal(free_sem.at[1], inc=1, device_id={"ep": at_chip(-1, core)}, device_id_type=MESH)
    pl.semaphore_signal(free_sem.at[2], inc=1, device_id={"ep": at_chip(1, core)}, device_id_type=MESH)

    def part_copy(chunk, rest):
        par = lax.rem(chunk, 2)
        which = pl.ds(0, far_pos) if rest else pl.ds(far_pos, 1)
        return pltpu.make_async_remote_copy(
            src_ref=part.at[par, which, 1 - core],
            dst_ref=from_core.at[chunk, which],
            send_sem=p_send.at[par],
            recv_sem=p_recv.at[chunk, rest],
            device_id={"ep": partner},
            device_id_type=MESH,
        )

    def part_sent(chunk):
        par = lax.rem(chunk, 2)
        wait_bytes(part.at[par, :, 0], p_send.at[par])

    def ring_copy(chunk, way, hop):
        dev = {"ep": at_chip(1 if way == 0 else -1, core)}
        if hop == 1:
            src = from_core.at[chunk, far_pos, pl.ds(way * half, half), :]
            dst = ring.at[chunk, way, 0, pl.ds(way * half, half), :]
        else:
            src = ring.at[chunk, way, hop - 2]
            dst = ring.at[chunk, way, hop - 1]
        return pltpu.make_async_remote_copy(
            src_ref=src,
            dst_ref=dst,
            send_sem=r_send.at[chunk],
            recv_sem=r_recv.at[chunk, hop - 1],
            device_id=dev,
            device_id_type=MESH,
        )

    def dest_pos(way, hops):
        return pos_of(1 - way, hops)

    def down(chunk):
        par = lax.rem(chunk, 2)
        for which in range(d_per):
            d_copy(chunk, which).wait()
        for e in range(n_exp):
            got = jnp.dot(hid[e * cap : (e + 1) * cap, :], dbuf[par * d_per + e], preferred_element_type=F32)
            erows[e * cap : (e + 1) * cap, :] = got.astype(BF16)
        shared = jnp.dot(shid[:, :inter], dbuf[par * d_per + n_exp], preferred_element_type=F32)
        shared = shared + jnp.dot(shid[:, inter:], dbuf[par * d_per + n_exp + 1], preferred_element_type=F32)
        sout[:, pl.ds(pl.multiple_of(chunk * COLS, COLS), COLS)] = shared.astype(BF16)

        @pl.when(chunk + 2 < n_chunks)
        def _():
            for which in range(d_per):
                d_copy(chunk + 2, which).start()

    def combine(chunk, groups):
        par = lax.rem(chunk, 2)
        for g in groups:
            rows = slice(g * group_rows, (g + 1) * group_rows)
            acc = None
            for e in range(n_exp):
                got = jnp.dot(
                    place[rows, e * cap : (e + 1) * cap], erows[e * cap : (e + 1) * cap, :], preferred_element_type=F32
                )
                got = cols_ref[rows, 8 + e : 9 + e] * got
                acc = got if acc is None else acc + got
            for b in range(4):
                part[par, 2 * g + b // 2, b % 2] = acc[b * tok : (b + 1) * tok]

    def fold_rest(chunk):
        par = lax.rem(chunk, 2)
        part_copy(chunk, 1).wait_recv()
        for pos in range(far_pos):
            from_core[chunk, pos] = from_core[chunk, pos] + part[par, pos, core]

    def first_hop(chunk):
        par = lax.rem(chunk, 2)
        part_copy(chunk, 0).wait_recv()
        from_core[chunk, far_pos] = from_core[chunk, far_pos] + part[par, far_pos, core]

        @pl.when(chunk == 0)
        def _():
            pl.semaphore_wait(free_sem.at[1], 1)
            pl.semaphore_wait(free_sem.at[2], 1)

        for way in (0, 1):
            ring_copy(chunk, way, 1).start()

    def ring_arrived(chunk, hop):
        wait_bytes(ring.at[chunk, 0, 0] if hop == 1 else ring.at[chunk, :, 0], r_recv.at[chunk, hop - 1])

    def pass_on(chunk, hop):
        ring_arrived(chunk, hop)
        for way in (0, 1):
            pos = dest_pos(way, far - hop)
            if hop == 1:
                done = pl.ds(way * half, half)
                rest = pl.ds((1 - way) * half, half)
                ring[chunk, way, 0, done, :] = ring[chunk, way, 0, done, :] + from_core[chunk, pos, done, :]
                ring[chunk, way, 0, rest, :] = from_core[chunk, pos, rest, :]
            else:
                ring[chunk, way, hop - 1] = ring[chunk, way, hop - 1] + from_core[chunk, pos]
            ring_copy(chunk, way, hop + 1).start()

    def finish(chunk):
        cols = pl.ds(pl.multiple_of(chunk * COLS, COLS), COLS)
        ring_arrived(chunk, far)
        routed = from_core[chunk, own_pos] + ring[chunk, 0, far - 1] + ring[chunk, 1, far - 1]
        out_ref[:, cols] = (hidden_ref[:, cols].astype(F32) + sout[:, cols].astype(F32) + routed).astype(BF16)

        @pl.when(chunk >= 1)
        def _():
            ring_sends_done(chunk - 1)

    def ring_sends_done(chunk):
        wait_bytes(from_core.at[chunk, pl.ds(0, 2 * far - 1)], r_send.at[chunk])

    def gather_sends_done():
        wait_bytes(xbuf.at[pl.ds(0, (chips - 1) * tok), :], ag_send)
        wait_bytes(xbuf.at[pl.ds(0, chips * tok), :], cc_send)
        wait_bytes(gsend.at[pl.ds(0, ep_size - 1)], g_send)

    def turn(i, carry):
        def for_chunk(lag, name, fn):
            @pl.when((i >= lag) & (i - lag < n_chunks))
            def _():
                with jax.named_scope(name):
                    fn(i - lag)

        def hops_of(in_middle):
            for hop in range(1, far + 1):
                if (hop % 2 == 0) == in_middle:
                    lag = 3 * hop // 2 if in_middle else (3 * hop - 1) // 2
                    if hop == far:
                        for_chunk(lag, "finish", finish)
                    else:
                        for_chunk(lag, "pass_on", functools.partial(pass_on, hop=hop))

        for_chunk(0, "down", down)
        for_chunk(1, "fold_rest", fold_rest)
        hops_of(True)

        @pl.when(i < n_chunks)
        def _():
            @pl.when(i >= 2)
            def _():
                part_sent(i)

            with jax.named_scope("combine_far"):
                combine(i, (n_groups - 1,))

                @pl.when(i == 0)
                def _():
                    pl.semaphore_wait(free_sem.at[0], 1)

                part_copy(i, 0).start()
            with jax.named_scope("combine"):
                combine(i, range(n_groups - 1))
                part_copy(i, 1).start()

        for_chunk(0, "first_hop", first_hop)
        hops_of(False)

        @pl.when(i == n_chunks)
        def _():
            gather_sends_done()

        return carry

    lax.fori_loop(0, n_chunks + 3 * far // 2, turn, 0)

    for par in (0, 1):
        part_sent(par)
    ring_sends_done(jnp.int32(n_chunks - 1))


def solution(mesh):
    ep_size = mesh.shape["ep"]

    def local_block(hidden_in, norm_gain, router_w, w_gate, w_up, w_down, ws_gate, ws_up, ws_down, expert_ids):
        tok, top_k = expert_ids.shape
        dim = hidden_in.shape[1]
        n_exp, _, inter = w_gate.shape
        s_inter = ws_gate.shape[1]
        chips = ep_size // 2
        far = chips // 2
        n_chunks = dim // COLS
        pair_cap = GROUPS * ((top_k + GROUP_LIMIT - 1) // GROUP_LIMIT) * tok // ep_size
        cap = pair_cap * ep_size // n_exp
        all_tok = ep_size * tok
        slots = n_exp * cap
        n_tiles = all_tok // LANES
        vmem = pl.BlockSpec(memory_space=pltpu.VMEM)
        hbm = pl.BlockSpec(memory_space=pl.ANY)
        dma = pltpu.SemaphoreType.DMA
        return pl.pallas_call(
            functools.partial(moe_kernel, ep_size, cap),
            out_shape=pltpu.VMEM((tok, dim), BF16),
            in_specs=[hbm] * 10,
            out_specs=vmem,
            scratch_shapes=[
                pltpu.VMEM((all_tok, dim), BF16),
                pltpu.VMEM((ep_size, 8, LANES), F32),
                pltpu.VMEM((chips, 2, 8, LANES), F32),
                pltpu.VMEM((n_tiles, 8, LANES), F32),
                pltpu.VMEM((all_tok, LANES), F32),
                pltpu.VMEM((slots, all_tok), BF16),
                pltpu.VMEM((all_tok, slots), BF16),
                pltpu.VMEM((slots, dim), BF16),
                pltpu.VMEM((slots, inter), BF16),
                pltpu.VMEM((tok, s_inter), BF16),
                pltpu.VMEM((tok, dim), BF16),
                pltpu.VMEM((STREAM_SLOTS, dim // 2, 2 * LANES), BF16),
                pltpu.VMEM((2 * (n_exp + 2), inter, COLS), BF16),
                pltpu.VMEM((2, chips, 2, tok, COLS), F32),
                pltpu.VMEM((slots, COLS), BF16),
                pltpu.VMEM((n_chunks, chips, tok, COLS), F32),
                pltpu.VMEM((n_chunks, 2, far, tok, COLS), F32),
                dma((STREAM_SLOTS,)),
                dma((2 * (n_exp + 2),)),
                dma,
                dma((far, 2, 2)),
                dma,
                dma((far + 1, 2)),
                dma,
                dma,
                dma((2,)),
                dma((n_chunks, 2)),
                dma((n_chunks,)),
                dma((n_chunks, far)),
                pltpu.VMEM((tok, dim), BF16),
                pltpu.VMEM((1, dim), F32),
                pltpu.VMEM(router_w.shape, F32),
                pltpu.VMEM((top_k, tok), jnp.int32),
                dma((4,)),
                pltpu.VMEM((n_exp, cap, COLS), F32),
                pltpu.SemaphoreType.REGULAR((3,)),
            ],
            compiler_params=pltpu.CompilerParams(
                collective_id=0, has_side_effects=True, vmem_limit_bytes=66500000
            ),
        )(hidden_in, norm_gain.reshape(1, dim), router_w, expert_ids.T, w_gate, w_up, w_down, ws_gate, ws_up, ws_down)

    row_spec = P(("dp", "ep"), None)
    in_specs = (row_spec, P(), P(), P("ep"), P("ep"), P("ep"), P(), P(), P(), row_spec)
    return jax.shard_map(local_block, mesh=mesh, in_specs=in_specs, out_specs=row_spec, check_vma=False)
```
